128 devices in a mesh: section: 4 (over y), wide: 8 (over z, x_hi), narrow: 4 (over x_lo, core).
Axes of the slice: x: 4 (x_hi: 2, x_lo: 2; x = x_hi * 2 + x_lo), y: 4, z: 4, core: 2. Of those that a mesh axis runs over, the one named last changes fastest.
Arguments:
- normed_inputs: bfloat16 [4, 4, 4, 768, 4096], P('section', 'narrow', None, 'wide'), may hold values from -160 to 160
- value_cotangent: bfloat16 [4, 4, 4, 768, 1024], P('section', 'narrow', None, 'wide'), may hold values from -6 to 6
- expert_hidden: bfloat16 [4, 4, 4, 256, 7168], P('section', 'narrow', None, None, 'wide'), may hold values from -40 to 40
- expert_cotangent: bfloat16 [4, 4, 4, 256, 4096], P('section', 'narrow', None, 'wide'), may hold values from -110 to 110
- slot_gate: bfloat16 [4, 4, 4, 256], P('section', 'narrow', None, 'wide'), may hold values from 0.25 to 1
- slot_count: int32 [4, 4, 4], P('section', 'narrow'), may hold values from 129 to 256, as said below
- expert_weight: bfloat16 [4, 7168, 4096], P('section', 'wide', 'narrow'), may hold values from -0.0625 to 0.0625
- expert_moment: float32 [4, 7168, 4096], P('section', 'wide', 'narrow'), may hold values from -6 to 6
- value_weight: bfloat16 [4, 4096, 1024], P('section', ('wide', 'narrow')), may hold values from -0.09375 to 0.09375
- value_moment: float32 [4, 4096, 1024], P('section', ('wide', 'narrow')), may hold values from -6 to 6
Outputs:
- expert_weight_next: bfloat16 [4, 7168, 4096], P('section', 'wide', 'narrow')
- expert_moment_next: float32 [4, 7168, 4096], P('section', 'wide', 'narrow')
- value_weight_next: bfloat16 [4, 4096, 1024], P('section', ('wide', 'narrow'))
- value_moment_next: float32 [4, 4096, 1024], P('section', ('wide', 'narrow'))
The draws below stay inside these ranges and needn't reach their ends.
Inputs may be any that keep to these rules, and one draw needn't show every extreme that they name: The live slots of a micro-batch are slots 0 to slot_count - 1; in every layer and replica some micro-batch fills all 256 slots.
All inputs are finite; a program needn't handle non-finite values.
Results may differ from the reference program's by a relative error of at most 0.014.
Values may be sent and summed in bfloat16 or wider, within the bound.
A program may use at most 128 MiB of HBM per device.

```python
import math
import jax
import jax.numpy as jnp
from jax import lax

D = 4096
FF = 7168
KV = 1024
MICRO = 4
MB_DEV = 96
SECTIONS = 4
REPLICAS = 4
SEQ = 768
SLOTS = 256
N_WIDE = 8


def rough_field(base_key, extent, section_rise, divisor):
    subkeys = jax.random.split(base_key, 3)
    columns = extent[-1]
    layers = extent[0]
    column_pos = jnp.arange(columns, dtype=jnp.float32) / max(columns - 1, 1)
    column_scale = jnp.exp(math.log(3.0) * column_pos + jax.random.uniform(subkeys[0], (columns,), jnp.float32, 0.0, math.log(3.3)))
    layer_pos = jnp.arange(layers, dtype=jnp.float32) / max(layers - 1, 1)
    layer_scale = jnp.exp(section_rise * math.log(3.0) * layer_pos).reshape(layers, 1, 1, 1, 1)
    row_scale = jnp.exp(jax.random.uniform(subkeys[1], extent[:-1] + (1,), jnp.float32, 0.0, math.log(3.0)))
    values = jnp.clip(jax.random.normal(subkeys[2], extent, jnp.float32), -6.0, 6.0)
    return values * row_scale * column_scale * layer_scale / divisor


def draw_normed_inputs(key, part):
    return rough_field(jax.random.fold_in(key, 3), (SECTIONS, REPLICAS, MICRO, SEQ, D), 1.0, 4.0).astype(jnp.bfloat16)


def draw_expert_hidden(key, part):
    return rough_field(jax.random.fold_in(key, 5), (SECTIONS, REPLICAS, MICRO, SLOTS, FF), 0.0, 6.0).astype(jnp.bfloat16)


def draw_expert_cotangent(key, part):
    return rough_field(jax.random.fold_in(key, 7), (SECTIONS, REPLICAS, MICRO, SLOTS, D), 1.0, 6.0).astype(jnp.bfloat16)


def draw_slot_count(key, part):
    count_key = jax.random.fold_in(key, 11)
    pick_key = jax.random.fold_in(key, 13)
    counts = jax.random.randint(count_key, (SECTIONS, REPLICAS, MICRO), SLOTS // 2 + 1, SLOTS + 1, dtype=jnp.int32)
    chosen = jax.random.randint(pick_key, (SECTIONS, REPLICAS, 1), 0, MICRO, dtype=jnp.int32)
    positions = jnp.arange(MICRO, dtype=jnp.int32).reshape(1, 1, MICRO)
    return jnp.where(positions == chosen, jnp.int32(SLOTS), counts).astype(jnp.int32)


def block_scale(key, dims, cuts, smallest, high):
    level = 1.0
    for position, parts in cuts:
        heights = jax.random.uniform(jax.random.fold_in(jax.random.fold_in(key, 6), position), (parts,), jnp.float32, smallest / len(cuts), high / len(cuts))
        level = level * jnp.repeat(jnp.exp(heights), dims[position] // parts).reshape((-1,) + (1,) * (len(dims) - 1 - position))
    return level


def scatter_about(key, shape, deviation, reach, shards=(), held_as=jnp.bfloat16):
    level = block_scale(key, shape, shards, -0.22, 0.18) if shards else 1.0
    entries = jax.random.normal(key, shape, jnp.float32) * deviation * level
    return jnp.minimum(jnp.maximum(entries, -reach), reach).astype(held_as)


def setup_inputs(seed: int = 0) -> dict:
    key_of = jax.random.split(jax.random.key(seed), 11)
    normed_inputs = draw_normed_inputs(jax.random.fold_in(key_of[10], 71), 0)
    value_cotangent = scatter_about(key_of[1], (SECTIONS, REPLICAS, MICRO, SEQ, KV), 1.0, 6.0, ((0, 4), (1, 4), (3, 8)))
    expert_hidden = draw_expert_hidden(jax.random.fold_in(key_of[10], 71), 0)
    expert_cotangent = draw_expert_cotangent(jax.random.fold_in(key_of[10], 71), 0)
    slot_gate = jnp.clip(0.25 + 0.75 * jax.random.uniform(key_of[4], (SECTIONS, REPLICAS, MICRO, SLOTS), jnp.float32) ** block_scale(key_of[4], (SECTIONS, REPLICAS, MICRO, SLOTS), ((0, 4), (1, 4), (3, 8)), -0.2, 0.2), 0.25, 1.0).astype(jnp.bfloat16)
    slot_count = draw_slot_count(jax.random.fold_in(key_of[10], 71), 0)
    expert_weight = scatter_about(key_of[6], (SECTIONS, FF, D), FF ** -0.5, 0.0625, ((0, 4), (1, 8), (2, 4)))
    expert_moment = scatter_about(key_of[7], (SECTIONS, FF, D), 1.0, 6.0, ((0, 4), (1, 8), (2, 4)), jnp.float32)
    value_weight = scatter_about(key_of[8], (SECTIONS, D, KV), D ** -0.5, 0.09375, ((0, 4), (1, 32)))
    value_moment = scatter_about(key_of[9], (SECTIONS, D, KV), 1.0, 6.0, ((0, 4), (1, 32)), jnp.float32)
    return {"normed_inputs": normed_inputs, "value_cotangent": value_cotangent, "expert_hidden": expert_hidden, "expert_cotangent": expert_cotangent, "slot_gate": slot_gate, "slot_count": slot_count, "expert_weight": expert_weight, "expert_moment": expert_moment, "value_weight": value_weight, "value_moment": value_moment}


MOMENTUM_DECAY = 0.9
STEP_RATE = 0.01

def rounded_add(accumulated, product):
    kept = lax.optimization_barrier(product.astype(jnp.bfloat16))
    return accumulated + kept.astype(jnp.float32)

def expert_layer(hidden_layer, cotangent_layer, gate_layer, count_layer):
    positions = jnp.arange(SLOTS, dtype=jnp.int32)
    live = positions[None, None, :] < count_layer[:, :, None]
    coefficient = jnp.where(live, gate_layer.astype(jnp.float32), jnp.zeros(gate_layer.shape, jnp.float32))
    scaled = (coefficient[..., None] * cotangent_layer.astype(jnp.float32)).astype(jnp.bfloat16)

    def add_replica(accumulated, pieces):
        hidden_rows = pieces[0].reshape(-1, FF)
        scaled_rows = pieces[1].reshape(-1, D)
        product = jnp.dot(hidden_rows.T, scaled_rows, preferred_element_type=jnp.float32)
        return (rounded_add(accumulated, product), None)
    result, ignored = lax.scan(add_replica, jnp.zeros((FF, D), jnp.float32), (hidden_layer, scaled))
    return result

def value_layer(input_layer, cotangent_layer):
    device_inputs = input_layer.reshape(REPLICAS, MICRO, N_WIDE, MB_DEV, D).transpose(0, 2, 1, 3, 4).reshape(REPLICAS * N_WIDE, MICRO * MB_DEV, D)
    device_cotangents = cotangent_layer.reshape(REPLICAS, MICRO, N_WIDE, MB_DEV, KV).transpose(0, 2, 1, 3, 4).reshape(REPLICAS * N_WIDE, MICRO * MB_DEV, KV)

    def add_device(accumulated, pieces):
        product = jnp.dot(pieces[0].T, pieces[1], preferred_element_type=jnp.float32)
        return (rounded_add(accumulated, product), None)
    result, ignored = lax.scan(add_device, jnp.zeros((D, KV), jnp.float32), (device_inputs, device_cotangents))
    return result

def reference(normed_inputs, value_cotangent, expert_hidden, expert_cotangent, slot_gate, slot_count, expert_weight, expert_moment, value_weight, value_moment):
    expert_grads = []
    value_grads = []
    for layer_index in range(SECTIONS):
        expert_grads.append(expert_layer(expert_hidden[layer_index], expert_cotangent[layer_index], slot_gate[layer_index], slot_count[layer_index]))
        value_grads.append(value_layer(normed_inputs[layer_index], value_cotangent[layer_index]))
    expert_grad = jnp.stack(expert_grads)
    value_grad = jnp.stack(value_grads)
    overall = jnp.sum(expert_grad * expert_grad) + jnp.sum(value_grad * value_grad)
    entry_count = SECTIONS * (FF * D + D * KV)
    factor = jnp.minimum(1.0, math.sqrt(entry_count) / jnp.sqrt(overall + 1e-06))
    expert_next = MOMENTUM_DECAY * expert_moment + factor * expert_grad
    value_next = MOMENTUM_DECAY * value_moment + factor * value_grad
    expert_weight_next = (expert_weight.astype(jnp.float32) - STEP_RATE * expert_next).astype(jnp.bfloat16)
    value_weight_next = (value_weight.astype(jnp.float32) - STEP_RATE * value_next).astype(jnp.bfloat16)
    return (expert_weight_next, expert_next, value_weight_next, value_next)
```

```python
import functools
import math

import jax
import jax.numpy as jnp
from jax import lax
from jax.experimental import pallas as pl
from jax.experimental.pallas import tpu as pltpu
from jax.sharding import Mesh
from jax.sharding import PartitionSpec as P

D = 4096
FF = 7168
KV = 1024
SECTIONS = 4
ENTRY_COUNT = SECTIONS * (FF * D + D * KV)
AXES = ("section", "wide_0", "wide_1", "narrow_0", "narrow_1")
WIDE = ("wide_0", "wide_1")
NARROW = ("narrow_0", "narrow_1")
WIDE_NARROW = ("wide_0", "wide_1", "narrow_0", "narrow_1")
MESH = pl.DeviceIdType.MESH

MOMENTUM_DECAY = 0.9
STEP_RATE = 0.01

PIECES = ((0, 0), (1, 0), (2, 0), (2, 1), (3, 0), (3, 1), (0, 1), (1, 1))
BY_Z1 = (0, 2, 4, 6)
BY_Z3 = (1, 3, 5, 7)


def flip(value, mask):
    if mask == 0:
        return value
    if mask == 1:
        return value + 1 - 2 * (value % 2)
    if mask == 2:
        return (value + 2) % 4
    return 3 - value


def kernel(
    count_ref, gate_ref, inputs, value_cot, hidden, cotangent,
    expert_out, value_out, factor_out,
    staged, gathered, relay, weights, tokens, token_cots, parts, halves, quarters, eighths, last,
    norms,
    local_sem, token_send, token_recv, cot_send, cot_recv, z_send, z_recv, zf_send, zf_recv,
    hid_send, hid_recv, val_send, val_recv, norm_send, norm_recv,
):
    section = lax.axis_index("section")
    z = lax.axis_index("wide_0")
    hi = lax.axis_index("wide_1")
    lo = lax.axis_index("narrow_0")
    core = lax.axis_index("narrow_1")
    x = 2 * hi + lo
    side = (hi, 1 - hi)

    def device(dy=0, dz=0, dx=0, dc=0):
        there = flip(x, dx)
        return (flip(section, dy), flip(z, dz), there // 2, there % 2, 1 - core if dc else core)

    def send(src, dst, send_sem, recv_sem, **where):
        return pltpu.make_async_remote_copy(
            src_ref=src, dst_ref=dst, send_sem=send_sem, recv_sem=recv_sem,
            device_id=device(**where), device_id_type=MESH,
        )

    pending = []

    def start(copy):
        copy.start()
        pending.append(copy)
        return copy

    peers = [dict(dx=i // 2, dc=i % 2) for i in range(1, 8)]
    peers += [dict(dz=i) for i in range(1, 4)] + [dict(dy=i) for i in range(1, 4)]

    cot_loads = []
    for rel in range(4):
        column = (2 * (1 - lo if rel // 2 else lo) + (1 - core if rel % 2 else core)) * 1024
        source = cotangent.at[:, :, pl.ds(pl.multiple_of(column, 1024), 1024)]
        load = pltpu.make_async_copy(source, staged.at[rel], local_sem.at[rel])
        load.start()
        cot_loads.append(load)
    barrier = pltpu.get_barrier_semaphore()
    for peer in peers:
        pl.semaphore_signal(barrier, inc=1, device_id=device(**peer), device_id_type=MESH)
    load_cots = pltpu.make_async_copy(value_cot, token_cots.at[0], local_sem.at[4])
    load_cots.start()
    others = []
    for dx in range(4):
        for dz in range(4):
            block = 2 * (4 * flip(z, dz) + flip(x, dx))
            place = pl.ds((dx * 4 + dz) * 128, 128)
            for which, owner in ((0, core), (1, 1 - core)):
                source = inputs.at[:, pl.ds(pl.multiple_of((block + owner) * 128, 128), 128)]
                if which == 0:
                    pltpu.make_async_copy(source, tokens.at[0, :, place], local_sem.at[5]).start()
                else:
                    others.append((source, place))
    hid_loads = []
    for dz in range(4):
        rows = pl.ds(pl.multiple_of(flip(z, dz) * 64, 64), 64)
        load = pltpu.make_async_copy(hidden.at[:, rows, :], weights.at[0, dz], local_sem.at[6 + dz])
        load.start()
        hid_loads.append(load)

    lanes = lax.broadcasted_iota(jnp.int32, (1, 32), 1) + (2 * z + hi) * 32
    diagonal = lax.broadcasted_iota(jnp.int32, (32, 32), 0) == lax.broadcasted_iota(
        jnp.int32, (32, 32), 1
    )
    columns = []
    for micro in range(4):
        gate = gate_ref[micro : micro + 1, :].astype(jnp.float32)
        row = jnp.where(lanes < count_ref[micro], gate, jnp.zeros_like(gate))
        square = jnp.where(diagonal, jnp.broadcast_to(row, (32, 32)), 0.0)
        columns.append(jnp.sum(square, axis=1, keepdims=True))
    for rel in range(4):
        cot_loads[rel].wait()
        for micro in range(4):
            scaled = (columns[micro] * staged[rel, micro].astype(jnp.float32)).astype(jnp.bfloat16)
            if rel == 0:
                gathered[0, 0, micro, hi] = scaled
            else:
                staged[rel, micro] = scaled

    pl.semaphore_wait(barrier, len(peers))

    def piece(slot, index):
        replica, far = PIECES[index]
        return gathered.at[slot, replica, :, side[far]]

    def along_z(index):
        start(send(piece(0, index), piece(1, index), z_send.at[0, index], z_recv.at[0, index], dz=1))
        start(send(piece(0, index), piece(3, index), z_send.at[1, index], z_recv.at[1, index], dz=3))

    def z_arrival(link, index):
        slot = (1, 3)[link]
        return send(piece(0, index), piece(slot, index), z_send.at[link, index], z_recv.at[link, index], dz=slot)

    def forward_z(index):
        if index in BY_Z1:
            z_arrival(1, index).wait_recv()
            start(send(piece(3, index), piece(2, index), zf_send.at[index], zf_recv.at[index], dz=1))
        else:
            z_arrival(0, index).wait_recv()
            start(send(piece(1, index), piece(2, index), zf_send.at[index], zf_recv.at[index], dz=3))

    def into(replica, far):
        return gathered.at[0, replica, :, side[far]]

    mine_0 = into(0, 0)
    cot = {}

    def cot_send_of(name, index, src, dst, **where):
        cot[name] = start(send(src, dst, cot_send.at[index], cot_recv.at[index], **where))

    cot_send_of("core", 0, staged.at[1], into(1, 0), dc=1)
    cot_send_of("relay_1", 1, mine_0, relay.at[0], dx=1)
    cot_send_of("relay_3", 2, staged.at[1], relay.at[1], dx=3)
    along_z(0)
    cot_send_of("x1_same", 3, staged.at[2], into(2, 0), dx=1)
    cot_send_of("x3_same", 4, staged.at[2], into(2, 0), dx=3)
    cot_send_of("x1_cross", 5, staged.at[3], into(3, 0), dx=1, dc=1)
    cot_send_of("x3_cross", 6, staged.at[3], into(3, 0), dx=3, dc=1)

    for source, place in others:
        send(source, tokens.at[1, :, place], token_send.at[0], token_recv.at[0], dc=1).start()
    token_whole = send(tokens.at[1], tokens.at[1], token_send.at[0], token_recv.at[0], dc=1)
    pending.append(token_whole)
    cots_whole = start(send(value_cot, token_cots.at[1], token_send.at[1], token_recv.at[1], dc=1))
    hid_core = []
    for dz in range(4):
        rows = pl.ds(pl.multiple_of(flip(z, dz) * 64, 64), 64)
        hid_core.append(
            start(send(hidden.at[:, rows, :], weights.at[1, dz], hid_send.at[0, dz], hid_recv.at[0, dz], dc=1))
        )

    cot["core"].wait_recv()
    along_z(1)

    load_cots.wait()
    pltpu.make_async_copy(tokens.at[0], tokens.at[0], local_sem.at[5]).wait()
    token_whole.wait_recv()
    cots_whole.wait_recv()

    def value_parts(dx):
        def block(dz, carry):
            place = pl.ds(pl.multiple_of((dx * 4 + dz) * 128, 128), 128)
            lhs = tokens[:, :, place].reshape(768, 128)
            rhs = token_cots[...].reshape(768, KV)
            product = lax.dot_general(
                lhs, rhs, (((0,), (0,)), ((), ())), preferred_element_type=jnp.float32
            )
            parts[dx, dz] = product.astype(jnp.bfloat16)
            return carry

        lax.fori_loop(0, 4, block, 0)

    value_parts(2)
    cot["relay_1"].wait_recv()
    cot_send_of("far_3", 7, relay.at[0], into(0, 0), dx=3)
    cot["relay_3"].wait_recv()
    cot_send_of("far_1", 8, relay.at[1], into(1, 1), dx=1, dc=1)
    hid_far = []
    for dz in (0, 1, 3, 2):
        hid_loads[dz].wait()
        hid_far.append(
            start(send(weights.at[0, dz], weights.at[2, dz], hid_send.at[1, dz], hid_recv.at[1, dz], dx=1))
        )
    value = {}

    def value_send(name, index, src, dst, **where):
        value[name] = start(send(src, dst, val_send.at[index], val_recv.at[index], **where))

    ORDER = (1, 2, 3, 0)
    value_parts(3)
    for i, dz in enumerate(ORDER):
        value_send(("x3", 1, dz), i, parts.at[2, dz], halves.at[1, dz], dx=3)
    cot["x1_same"].wait_recv()
    along_z(2)
    cot["x3_same"].wait_recv()
    along_z(3)
    value_parts(1)
    for i, dz in enumerate(ORDER):
        value_send(("x3", 0, dz), 4 + i, parts.at[3, dz], halves.at[0, dz], dx=3)
    cot["x1_cross"].wait_recv()
    along_z(4)
    cot["x3_cross"].wait_recv()
    along_z(5)
    value_parts(0)
    forward_z(0)
    forward_z(1)
    cot["far_3"].wait_recv()
    along_z(6)
    cot["far_1"].wait_recv()
    along_z(7)

    def products(slot, replica, first=False):
        def tile(n, carry):
            place = pl.ds(pl.multiple_of(n * 256, 256), 256)
            lhs = weights[replica, slot].reshape(256, 896)
            rhs = gathered[slot, replica, :, :, :, place].reshape(256, 256)
            product = lax.dot_general(
                lhs, rhs, (((0,), (0,)), ((), ())), preferred_element_type=jnp.float32
            )
            if first:
                expert_out[:, place] = product
            else:
                expert_out[:, place] += product
            return carry

        lax.fori_loop(0, 4, tile, 0)

    products(0, 0, first=True)
    hid_core[0].wait_recv()
    products(0, 1)
    forward_z(2)
    forward_z(3)

    def second_step(dz):
        value[("x3", 1, dz)].wait_recv()
        total = parts[1, dz].astype(jnp.float32) + halves[1, dz].astype(jnp.float32)
        parts[1, dz] = total.astype(jnp.bfloat16)

    def second_send(dz):
        value_send(("x1", dz), 8 + dz, parts.at[1, dz], quarters.at[dz], dx=1)

    hid_pass = {}

    def pass_hidden(k):
        dz = (0, 1, 3, 2)[k]
        hid_far[k].wait_recv()
        hid_pass[dz] = start(
            send(weights.at[2, dz], weights.at[3, dz], hid_send.at[2, dz], hid_recv.at[2, dz], dc=1)
        )

    second_step(1)
    pass_hidden(0)
    second_send(1)
    forward_z(4)
    products(0, 2)
    second_step(2)
    forward_z(5)
    second_send(2)
    hid_pass[0].wait_recv()
    products(0, 3)
    second_step(3)
    pass_hidden(1)
    second_send(3)
    forward_z(6)
    forward_z(7)
    second_step(0)
    z_arrival(0, 0).wait_recv()
    z_arrival(0, 6).wait_recv()
    products(1, 0)
    second_send(0)
    hid_core[1].wait_recv()
    products(1, 1)
    z_arrival(1, 1).wait_recv()
    z_arrival(1, 7).wait_recv()
    z_arrival(0, 2).wait_recv()
    products(1, 2)
    hid_pass[1].wait_recv()
    z_arrival(0, 4).wait_recv()
    products(1, 3)
    pass_hidden(2)
    products(3, 0)
    hid_core[3].wait_recv()
    products(3, 1)
    z_arrival(1, 3).wait_recv()
    products(3, 2)
    hid_pass[3].wait_recv()
    z_arrival(1, 5).wait_recv()
    products(3, 3)

    def far_arrival(index):
        if index in BY_Z1:
            send(piece(3, index), piece(2, index), zf_send.at[index], zf_recv.at[index], dz=1).wait_recv()
        else:
            send(piece(1, index), piece(2, index), zf_send.at[index], zf_recv.at[index], dz=3).wait_recv()

    def third_step(dz):
        value[("x3", 0, dz)].wait_recv()
        value[("x1", dz)].wait_recv()
        return (
            parts[0, dz].astype(jnp.float32)
            + halves[0, dz].astype(jnp.float32)
            + quarters[dz].astype(jnp.float32)
        )

    pass_hidden(3)
    far_arrival(2)
    far_arrival(3)
    products(2, 2)
    parts[0, 1] = third_step(1).astype(jnp.bfloat16)
    far_arrival(4)
    far_arrival(5)
    hid_pass[2].wait_recv()
    products(2, 3)
    value_send("z1_0", 12, parts.at[0, 1], eighths.at[0], dz=1)
    parts[0, 2] = third_step(2).astype(jnp.bfloat16)
    far_arrival(0)
    far_arrival(6)
    products(2, 0)
    value_send("z1_1", 13, parts.at[0, 2], eighths.at[1], dz=1)
    hid_core[2].wait_recv()
    far_arrival(1)
    far_arrival(7)
    products(2, 1)

    def squares(ref, rows):
        def tile(i, total):
            chunk = ref[pl.ds(pl.multiple_of(i * 8, 8), 8), :]
            for n in range(8):
                one = chunk[:, n * 128 : (n + 1) * 128]
                total = total + one * one
            return total

        return lax.fori_loop(0, rows // 8, tile, jnp.zeros((8, 128), jnp.float32))

    expert_squares = squares(expert_out, 896)
    third = third_step(3)
    value["z1_1"].wait_recv()
    parts[0, 3] = (third + eighths[1].astype(jnp.float32)).astype(jnp.bfloat16)
    value_send("z3", 14, parts.at[0, 3], last, dz=3)
    near = third_step(0)
    value["z1_0"].wait_recv()
    near = near + eighths[0].astype(jnp.float32)
    value["z3"].wait_recv()
    value_out[...] = near + last[...].astype(jnp.float32)
    norms[0] = expert_squares + squares(value_out, 128)

    base = 0
    slot = 1
    for group in (peers[:7], peers[7:10], peers[10:]):
        copies = []
        for i, peer in enumerate(group):
            copies.append(
                start(
                    send(norms.at[base], norms.at[slot + i], norm_send.at[slot + i], norm_recv.at[slot + i], **peer)
                )
            )
        total = norms[base]
        for i, copy in enumerate(copies):
            copy.wait_recv()
            total = total + norms[slot + i]
        base = slot + len(group)
        norms[base] = total
        slot = base + 1
    overall = jnp.sum(jnp.sum(norms[base], axis=0, keepdims=True), axis=1, keepdims=True)
    overall = jnp.broadcast_to(overall, (8, 128))
    factor_out[...] = jnp.minimum(1.0, math.sqrt(ENTRY_COUNT) / jnp.sqrt(overall + 1e-06))

    for copy in pending:
        copy.wait_send()


def on_device(
    normed_inputs, value_cotangent, expert_hidden, expert_cotangent, slot_gate, slot_count,
    expert_weight, expert_moment, value_weight, value_moment,
):
    bf16 = jnp.bfloat16
    any_space = pl.BlockSpec(memory_space=pl.ANY)
    vmem = pl.BlockSpec(memory_space=pltpu.VMEM)
    dma = pltpu.SemaphoreType.DMA
    expert_grad, value_grad, factor = pl.pallas_call(
        kernel,
        name="gradients",
        out_shape=(
            jax.ShapeDtypeStruct((896, 1024), jnp.float32),
            jax.ShapeDtypeStruct((128, 1024), jnp.float32),
            jax.ShapeDtypeStruct((8, 128), jnp.float32),
        ),
        in_specs=[pl.BlockSpec(memory_space=pltpu.SMEM), vmem] + [any_space] * 4,
        out_specs=(vmem, vmem, vmem),
        scratch_shapes=[
            pltpu.VMEM((4, 4, 32, 1024), bf16),
            pltpu.VMEM((4, 4, 4, 2, 32, 1024), bf16),
            pltpu.VMEM((2, 4, 32, 1024), bf16),
            pltpu.VMEM((4, 4, 4, 64, 896), bf16),
            pltpu.VMEM((2, 384, 2048), bf16),
            pltpu.VMEM((2, 384, 1024), bf16),
            pltpu.VMEM((4, 4, 128, 1024), bf16),
            pltpu.VMEM((2, 4, 128, 1024), bf16),
            pltpu.VMEM((4, 128, 1024), bf16),
            pltpu.VMEM((2, 128, 1024), bf16),
            pltpu.VMEM((128, 1024), bf16),
            pltpu.VMEM((17, 8, 128), jnp.float32),
            dma((10,)),
            dma((2,)), dma((2,)),
            dma((9,)), dma((9,)),
            dma((2, 8)), dma((2, 8)),
            dma((8,)), dma((8,)),
            dma((3, 4)), dma((3, 4)),
            dma((15,)), dma((15,)),
            dma((17,)), dma((17,)),
        ],
        compiler_params=pltpu.CompilerParams(
            collective_id=0, has_side_effects=True, vmem_limit_bytes=46 * 1024 * 1024
        ),
        cost_estimate=pl.CostEstimate(
            flops=2 * 896 * 1024 * 4096 + 2 * 2048 * 1024 * 768,
            bytes_accessed=10_000_000,
            transcendentals=0,
        ),
    )(
        slot_count[0, 0],
        slot_gate[0, 0],
        normed_inputs[0, 0].reshape(384, D),
        value_cotangent[0, 0].reshape(384, KV),
        expert_hidden[0, 0],
        expert_cotangent[0, 0],
    )
    factor = factor[0, 0]
    expert_next = MOMENTUM_DECAY * expert_moment[0] + factor * expert_grad
    value_next = MOMENTUM_DECAY * value_moment[0] + factor * value_grad
    expert_weight_next = (expert_weight[0].astype(jnp.float32) - STEP_RATE * expert_next).astype(bf16)
    value_weight_next = (value_weight[0].astype(jnp.float32) - STEP_RATE * value_next).astype(bf16)
    return (expert_weight_next[None], expert_next[None], value_weight_next[None], value_next[None])


def solution(mesh):
    finer = Mesh(mesh.devices.reshape(mesh.shape["section"], 4, 2, 2, 2), AXES)
    specs = (
        P("section", WIDE, NARROW),
        P("section", WIDE, NARROW),
        P("section", WIDE_NARROW, None),
        P("section", WIDE_NARROW, None),
    )
    in_specs = (
        P("section", NARROW, None, WIDE, None),
        P("section", NARROW, None, WIDE, None),
        P("section", NARROW, None, None, WIDE),
        P("section", NARROW, None, WIDE, None),
        P("section", NARROW, None, WIDE),
        P("section", NARROW, None),
    ) + specs
    return jax.shard_map(
        on_device, mesh=finer, in_specs=in_specs, out_specs=specs, check_vma=False
    )
```

```python
import math

import jax
import jax.numpy as jnp
from jax import lax
from jax.experimental import pallas as pl
from jax.experimental.pallas import tpu as pltpu
from jax.sharding import Mesh
from jax.sharding import PartitionSpec as P

D = 4096
FF = 7168
KV = 1024
SECTIONS = 4
ENTRY_COUNT = SECTIONS * (FF * D + D * KV)
AXES = ("section", "wide_0", "wide_1", "narrow_0", "narrow_1")
WIDE = ("wide_0", "wide_1")
NARROW = ("narrow_0", "narrow_1")
WIDE_NARROW = ("wide_0", "wide_1", "narrow_0", "narrow_1")
MESH = pl.DeviceIdType.MESH

MOMENTUM_DECAY = 0.9
STEP_RATE = 0.01

PIECES = ((0, 0), (1, 0), (2, 0), (2, 1), (3, 0), (3, 1), (0, 1), (1, 1))
BY_Z1 = (0, 2, 4, 6)
BY_Z3 = (1, 3, 5, 7)


def flip(value, mask):
    if mask == 0:
        return value
    if mask == 1:
        return value + 1 - 2 * (value % 2)
    if mask == 2:
        return (value + 2) % 4
    return 3 - value


def kernel(
    counts, gates, inputs, value_cot, hidden, cotangent,
    expert_out, value_out, factor_out,
    count_ref, gate_ref, staged, gathered, relay, weights, tokens, token_cots, parts, halves, quarters, eighths, last,
    norms,
    local_sem, token_send, token_recv, cot_send, cot_recv, z_send, z_recv, zf_send, zf_recv,
    hid_send, hid_recv, val_send, val_recv, norm_send, norm_recv,
):
    section = lax.axis_index("section")
    z = lax.axis_index("wide_0")
    hi = lax.axis_index("wide_1")
    lo = lax.axis_index("narrow_0")
    core = lax.axis_index("narrow_1")
    x = 2 * hi + lo
    side = (hi, 1 - hi)

    def device(dy=0, dz=0, dx=0, dc=0):
        there = flip(x, dx)
        return (flip(section, dy), flip(z, dz), there // 2, there % 2, 1 - core if dc else core)

    def send(src, dst, send_sem, recv_sem, **where):
        return pltpu.make_async_remote_copy(
            src_ref=src, dst_ref=dst, send_sem=send_sem, recv_sem=recv_sem,
            device_id=device(**where), device_id_type=MESH,
        )

    pending = []

    def start(copy):
        copy.start()
        pending.append(copy)
        return copy

    peers = [dict(dx=i // 2, dc=i % 2) for i in range(1, 8)]
    peers += [dict(dz=i) for i in range(1, 4)] + [dict(dy=i) for i in range(1, 4)]

    small_loads = [
        pltpu.make_async_copy(counts, count_ref, local_sem.at[10]),
        pltpu.make_async_copy(gates, gate_ref, local_sem.at[11]),
    ]
    for load in small_loads:
        load.start()
    cot_loads = []
    for rel in range(4):
        column = (2 * (1 - lo if rel // 2 else lo) + (1 - core if rel % 2 else core)) * 1024
        source = cotangent.at[:, :, pl.ds(pl.multiple_of(column, 1024), 1024)]
        load = pltpu.make_async_copy(source, staged.at[rel], local_sem.at[rel])
        load.start()
        cot_loads.append(load)
    barrier = pltpu.get_barrier_semaphore()
    for peer in peers:
        pl.semaphore_signal(barrier, inc=1, device_id=device(**peer), device_id_type=MESH)
    load_cots = pltpu.make_async_copy(value_cot, token_cots.at[0], local_sem.at[4])
    load_cots.start()
    others = []
    for dx in range(4):
        for dz in range(4):
            block = 2 * (4 * flip(z, dz) + flip(x, dx))
            place = pl.ds((dx * 4 + dz) * 128, 128)
            for which, owner in ((0, core), (1, 1 - core)):
                source = inputs.at[:, pl.ds(pl.multiple_of((block + owner) * 128, 128), 128)]
                if which == 0:
                    pltpu.make_async_copy(source, tokens.at[0, :, place], local_sem.at[5]).start()
                else:
                    others.append((source, place))
    hid_loads = []
    for dz in range(4):
        rows = pl.ds(pl.multiple_of(flip(z, dz) * 64, 64), 64)
        load = pltpu.make_async_copy(hidden.at[:, rows, :], weights.at[0, dz], local_sem.at[6 + dz])
        load.start()
        hid_loads.append(load)

    lanes = lax.broadcasted_iota(jnp.int32, (1, 32), 1) + (2 * z + hi) * 32
    diagonal = lax.broadcasted_iota(jnp.int32, (32, 32), 0) == lax.broadcasted_iota(
        jnp.int32, (32, 32), 1
    )
    columns = []
    for load in small_loads:
        load.wait()
    for micro in range(4):
        gate = gate_ref[micro : micro + 1, :].astype(jnp.float32)
        row = jnp.where(lanes < count_ref[micro], gate, jnp.zeros_like(gate))
        square = jnp.where(diagonal, jnp.broadcast_to(row, (32, 32)), 0.0)
        columns.append(jnp.sum(square, axis=1, keepdims=True))
    for rel in range(4):
        cot_loads[rel].wait()
        for micro in range(4):
            scaled = (columns[micro] * staged[rel, micro].astype(jnp.float32)).astype(jnp.bfloat16)
            if rel == 0:
                gathered[0, 0, micro, hi] = scaled
            else:
                staged[rel, micro] = scaled

    pl.semaphore_wait(barrier, len(peers))

    def piece(slot, index):
        replica, far = PIECES[index]
        return gathered.at[slot, replica, :, side[far]]

    def along_z(index):
        start(send(piece(0, index), piece(1, index), z_send.at[0, index], z_recv.at[0, index], dz=1))
        start(send(piece(0, index), piece(3, index), z_send.at[1, index], z_recv.at[1, index], dz=3))

    def z_arrival(link, index):
        slot = (1, 3)[link]
        return send(piece(0, index), piece(slot, index), z_send.at[link, index], z_recv.at[link, index], dz=slot)

    def forward_z(index):
        if index in BY_Z1:
            z_arrival(1, index).wait_recv()
            start(send(piece(3, index), piece(2, index), zf_send.at[index], zf_recv.at[index], dz=1))
        else:
            z_arrival(0, index).wait_recv()
            start(send(piece(1, index), piece(2, index), zf_send.at[index], zf_recv.at[index], dz=3))

    def into(replica, far):
        return gathered.at[0, replica, :, side[far]]

    mine_0 = into(0, 0)
    cot = {}

    def cot_send_of(name, index, src, dst, **where):
        cot[name] = start(send(src, dst, cot_send.at[index], cot_recv.at[index], **where))

    cot_send_of("core", 0, staged.at[1], into(1, 0), dc=1)
    cot_send_of("relay_1", 1, mine_0, relay.at[0], dx=1)
    cot_send_of("relay_3", 2, staged.at[1], relay.at[1], dx=3)
    along_z(0)
    cot_send_of("x1_same", 3, staged.at[2], into(2, 0), dx=1)
    cot_send_of("x3_same", 4, staged.at[2], into(2, 0), dx=3)
    cot_send_of("x1_cross", 5, staged.at[3], into(3, 0), dx=1, dc=1)
    cot_send_of("x3_cross", 6, staged.at[3], into(3, 0), dx=3, dc=1)

    for source, place in others:
        send(source, tokens.at[1, :, place], token_send.at[0], token_recv.at[0], dc=1).start()
    token_whole = send(tokens.at[1], tokens.at[1], token_send.at[0], token_recv.at[0], dc=1)
    pending.append(token_whole)
    cots_whole = start(send(value_cot, token_cots.at[1], token_send.at[1], token_recv.at[1], dc=1))
    hid_core = []
    for dz in range(4):
        rows = pl.ds(pl.multiple_of(flip(z, dz) * 64, 64), 64)
        hid_core.append(
            start(send(hidden.at[:, rows, :], weights.at[1, dz], hid_send.at[0, dz], hid_recv.at[0, dz], dc=1))
        )

    cot["core"].wait_recv()
    along_z(1)

    load_cots.wait()
    pltpu.make_async_copy(tokens.at[0], tokens.at[0], local_sem.at[5]).wait()
    token_whole.wait_recv()
    cots_whole.wait_recv()

    def value_parts(dx):
        def block(dz, carry):
            place = pl.ds(pl.multiple_of((dx * 4 + dz) * 128, 128), 128)
            lhs = tokens[:, :, place].reshape(768, 128)
            rhs = token_cots[...].reshape(768, KV)
            product = lax.dot_general(
                lhs, rhs, (((0,), (0,)), ((), ())), preferred_element_type=jnp.float32
            )
            parts[dx, dz] = product.astype(jnp.bfloat16)
            return carry

        lax.fori_loop(0, 4, block, 0)

    value_parts(2)
    cot["relay_1"].wait_recv()
    cot_send_of("far_3", 7, relay.at[0], into(0, 0), dx=3)
    cot["relay_3"].wait_recv()
    cot_send_of("far_1", 8, relay.at[1], into(1, 1), dx=1, dc=1)
    hid_far = []
    for dz in (0, 1, 3, 2):
        hid_loads[dz].wait()
        hid_far.append(
            start(send(weights.at[0, dz], weights.at[2, dz], hid_send.at[1, dz], hid_recv.at[1, dz], dx=1))
        )
    value = {}

    def value_send(name, index, src, dst, **where):
        value[name] = start(send(src, dst, val_send.at[index], val_recv.at[index], **where))

    ORDER = (1, 2, 3, 0)
    value_parts(3)
    for i, dz in enumerate(ORDER):
        value_send(("x3", 1, dz), i, parts.at[2, dz], halves.at[1, dz], dx=3)
    cot["x1_same"].wait_recv()
    along_z(2)
    cot["x3_same"].wait_recv()
    along_z(3)
    value_parts(1)
    for i, dz in enumerate(ORDER):
        value_send(("x3", 0, dz), 4 + i, parts.at[3, dz], halves.at[0, dz], dx=3)
    cot["x1_cross"].wait_recv()
    along_z(4)
    cot["x3_cross"].wait_recv()
    along_z(5)
    value_parts(0)
    forward_z(0)
    forward_z(1)
    cot["far_3"].wait_recv()
    along_z(6)
    cot["far_1"].wait_recv()
    along_z(7)

    def products(slot, replica, first=False):
        def tile(n, carry):
            place = pl.ds(pl.multiple_of(n * 256, 256), 256)
            lhs = weights[replica, slot].reshape(256, 896)
            rhs = gathered[slot, replica, :, :, :, place].reshape(256, 256)
            product = lax.dot_general(
                lhs, rhs, (((0,), (0,)), ((), ())), preferred_element_type=jnp.float32
            )
            if first:
                expert_out[:, place] = product
            else:
                expert_out[:, place] += product
            return carry

        lax.fori_loop(0, 4, tile, 0)

    products(0, 0, first=True)
    hid_core[0].wait_recv()
    products(0, 1)
    forward_z(2)
    forward_z(3)

    def second_step(dz):
        value[("x3", 1, dz)].wait_recv()
        total = parts[1, dz].astype(jnp.float32) + halves[1, dz].astype(jnp.float32)
        parts[1, dz] = total.astype(jnp.bfloat16)

    def second_send(dz):
        value_send(("x1", dz), 8 + dz, parts.at[1, dz], quarters.at[dz], dx=1)

    hid_pass = {}

    def pass_hidden(k):
        dz = (0, 1, 3, 2)[k]
        hid_far[k].wait_recv()
        hid_pass[dz] = start(
            send(weights.at[2, dz], weights.at[3, dz], hid_send.at[2, dz], hid_recv.at[2, dz], dc=1)
        )

    second_step(1)
    pass_hidden(0)
    second_send(1)
    forward_z(4)
    products(0, 2)
    second_step(2)
    forward_z(5)
    second_send(2)
    hid_pass[0].wait_recv()
    products(0, 3)
    second_step(3)
    pass_hidden(1)
    second_send(3)
    forward_z(6)
    forward_z(7)
    second_step(0)
    z_arrival(0, 0).wait_recv()
    z_arrival(0, 6).wait_recv()
    products(1, 0)
    second_send(0)
    hid_core[1].wait_recv()
    products(1, 1)
    z_arrival(1, 1).wait_recv()
    z_arrival(1, 7).wait_recv()
    z_arrival(0, 2).wait_recv()
    products(1, 2)
    hid_pass[1].wait_recv()
    z_arrival(0, 4).wait_recv()
    products(1, 3)
    pass_hidden(2)
    products(3, 0)
    hid_core[3].wait_recv()
    products(3, 1)
    z_arrival(1, 3).wait_recv()
    products(3, 2)
    hid_pass[3].wait_recv()
    z_arrival(1, 5).wait_recv()
    products(3, 3)

    def far_arrival(index):
        if index in BY_Z1:
            send(piece(3, index), piece(2, index), zf_send.at[index], zf_recv.at[index], dz=1).wait_recv()
        else:
            send(piece(1, index), piece(2, index), zf_send.at[index], zf_recv.at[index], dz=3).wait_recv()

    def third_step(dz):
        value[("x3", 0, dz)].wait_recv()
        value[("x1", dz)].wait_recv()
        return (
            parts[0, dz].astype(jnp.float32)
            + halves[0, dz].astype(jnp.float32)
            + quarters[dz].astype(jnp.float32)
        )

    pass_hidden(3)
    far_arrival(2)
    far_arrival(3)
    products(2, 2)
    parts[0, 1] = third_step(1).astype(jnp.bfloat16)
    far_arrival(4)
    far_arrival(5)
    hid_pass[2].wait_recv()
    products(2, 3)
    value_send("z1_0", 12, parts.at[0, 1], eighths.at[0], dz=1)
    parts[0, 2] = third_step(2).astype(jnp.bfloat16)
    far_arrival(0)
    far_arrival(6)
    products(2, 0)
    value_send("z1_1", 13, parts.at[0, 2], eighths.at[1], dz=1)
    hid_core[2].wait_recv()
    far_arrival(1)
    far_arrival(7)
    products(2, 1)

    def squares(ref, rows):
        def tile(i, total):
            chunk = ref[pl.ds(pl.multiple_of(i * 8, 8), 8), :]
            for n in range(8):
                one = chunk[:, n * 128 : (n + 1) * 128]
                total = total + one * one
            return total

        return lax.fori_loop(0, rows // 8, tile, jnp.zeros((8, 128), jnp.float32))

    expert_squares = squares(expert_out, 896)
    third = third_step(3)
    value["z1_1"].wait_recv()
    parts[0, 3] = (third + eighths[1].astype(jnp.float32)).astype(jnp.bfloat16)
    value_send("z3", 14, parts.at[0, 3], last, dz=3)
    near = third_step(0)
    value["z1_0"].wait_recv()
    near = near + eighths[0].astype(jnp.float32)
    value["z3"].wait_recv()
    value_out[...] = near + last[...].astype(jnp.float32)
    norms[0] = expert_squares + squares(value_out, 128)

    base = 0
    slot = 1
    for group in (peers[:7], peers[7:10], peers[10:]):
        copies = []
        for i, peer in enumerate(group):
            copies.append(
                start(
                    send(norms.at[base], norms.at[slot + i], norm_send.at[slot + i], norm_recv.at[slot + i], **peer)
                )
            )
        total = norms[base]
        for i, copy in enumerate(copies):
            copy.wait_recv()
            total = total + norms[slot + i]
        base = slot + len(group)
        norms[base] = total
        slot = base + 1
    overall = jnp.sum(jnp.sum(norms[base], axis=0, keepdims=True), axis=1, keepdims=True)
    overall = jnp.broadcast_to(overall, (8, 128))
    factor_out[...] = jnp.minimum(1.0, math.sqrt(ENTRY_COUNT) / jnp.sqrt(overall + 1e-06))

    for copy in pending:
        copy.wait_send()


def update_kernel(
    factor_ref, expert_grad, expert_moment, expert_weight, value_grad, value_moment, value_weight,
    expert_weight_out, expert_moment_out, value_weight_out, value_moment_out,
    new_weights, new_moments, weight_sem, moment_sem,
):
    factor = factor_ref[0:1, 0:1]
    copies = []
    for tile in range(8):
        rows = pl.ds(tile * 128, 128)
        if tile < 7:
            there, refs = rows, (expert_grad, expert_moment, expert_weight)
            outs = (expert_weight_out, expert_moment_out)
        else:
            there, refs = pl.ds(0, 128), (value_grad, value_moment, value_weight)
            outs = (value_weight_out, value_moment_out)

        def chunk(i, carry, tile=tile, refs=refs):
            grad, moment, weight = refs
            at = pl.ds(pl.multiple_of((tile % 7) * 128 + i * 16, 16), 16)
            to = pl.ds(pl.multiple_of(tile * 128 + i * 16, 16), 16)
            moved = MOMENTUM_DECAY * moment[at, :] + factor * grad[at, :]
            new_moments[to, :] = moved
            new_weights[to, :] = (weight[at, :].astype(jnp.float32) - STEP_RATE * moved).astype(
                jnp.bfloat16
            )
            return carry

        lax.fori_loop(0, 8, chunk, 0)
        for src, dst, sem in (
            (new_weights, outs[0], weight_sem),
            (new_moments, outs[1], moment_sem),
        ):
            copy = pltpu.make_async_copy(src.at[rows, :], dst.at[there, :], sem.at[tile])
            copy.start()
            copies.append(copy)
    for copy in copies:
        copy.wait()


def on_device(
    normed_inputs, value_cotangent, expert_hidden, expert_cotangent, slot_gate, slot_count,
    expert_weight, expert_moment, value_weight, value_moment,
):
    bf16 = jnp.bfloat16
    in_hbm = pl.BlockSpec(memory_space=pltpu.HBM)
    vmem = pl.BlockSpec(memory_space=pltpu.VMEM)
    dma = pltpu.SemaphoreType.DMA
    expert_grad, value_grad, factor = pl.pallas_call(
        kernel,
        name="gradients",
        out_shape=(
            pltpu.VMEM((896, 1024), jnp.float32),
            pltpu.VMEM((128, 1024), jnp.float32),
            pltpu.VMEM((8, 128), jnp.float32),
        ),
        in_specs=[in_hbm] * 6,
        out_specs=(vmem, vmem, vmem),
        scratch_shapes=[
            pltpu.SMEM((4,), jnp.int32),
            pltpu.VMEM((4, 32), bf16),
            pltpu.VMEM((4, 4, 32, 1024), bf16),
            pltpu.VMEM((4, 4, 4, 2, 32, 1024), bf16),
            pltpu.VMEM((2, 4, 32, 1024), bf16),
            pltpu.VMEM((4, 4, 4, 64, 896), bf16),
            pltpu.VMEM((2, 384, 2048), bf16),
            pltpu.VMEM((2, 384, 1024), bf16),
            pltpu.VMEM((4, 4, 128, 1024), bf16),
            pltpu.VMEM((2, 4, 128, 1024), bf16),
            pltpu.VMEM((4, 128, 1024), bf16),
            pltpu.VMEM((2, 128, 1024), bf16),
            pltpu.VMEM((128, 1024), bf16),
            pltpu.VMEM((17, 8, 128), jnp.float32),
            dma((12,)),
            dma((2,)), dma((2,)),
            dma((9,)), dma((9,)),
            dma((2, 8)), dma((2, 8)),
            dma((8,)), dma((8,)),
            dma((3, 4)), dma((3, 4)),
            dma((15,)), dma((15,)),
            dma((17,)), dma((17,)),
        ],
        compiler_params=pltpu.CompilerParams(
            collective_id=0, has_side_effects=True, vmem_limit_bytes=46 * 1024 * 1024
        ),
        cost_estimate=pl.CostEstimate(
            flops=2 * 896 * 1024 * 4096 + 2 * 2048 * 1024 * 768,
            bytes_accessed=10_000_000,
            transcendentals=0,
        ),
    )(
        pltpu.with_memory_space_constraint(slot_count[0, 0], pltpu.HBM),
        pltpu.with_memory_space_constraint(slot_gate[0, 0], pltpu.HBM),
        pltpu.with_memory_space_constraint(normed_inputs[0, 0].reshape(384, D), pltpu.HBM),
        pltpu.with_memory_space_constraint(value_cotangent[0, 0].reshape(384, KV), pltpu.HBM),
        pltpu.with_memory_space_constraint(expert_hidden[0, 0], pltpu.HBM),
        pltpu.with_memory_space_constraint(expert_cotangent[0, 0], pltpu.HBM),
    )
    expert_weight_next, expert_next, value_weight_next, value_next = pl.pallas_call(
        update_kernel,
        name="update",
        out_shape=(
            jax.ShapeDtypeStruct((896, 1024), bf16),
            jax.ShapeDtypeStruct((896, 1024), jnp.float32),
            jax.ShapeDtypeStruct((128, 1024), bf16),
            jax.ShapeDtypeStruct((128, 1024), jnp.float32),
        ),
        in_specs=[vmem] * 7,
        out_specs=(in_hbm,) * 4,
        scratch_shapes=[
            pltpu.VMEM((1024, 1024), bf16),
            pltpu.VMEM((1024, 1024), jnp.float32),
            dma((8,)),
            dma((8,)),
        ],
        compiler_params=pltpu.CompilerParams(vmem_limit_bytes=24 * 1024 * 1024),
        cost_estimate=pl.CostEstimate(flops=6 * 1024 * 1024, bytes_accessed=6_000_000, transcendentals=0),
    )(
        factor, expert_grad, expert_moment[0], expert_weight[0],
        value_grad, value_moment[0], value_weight[0],
    )
    return (expert_weight_next[None], expert_next[None], value_weight_next[None], value_next[None])


def solution(mesh):
    finer = Mesh(mesh.devices.reshape(mesh.shape["section"], 4, 2, 2, 2), AXES)
    specs = (
        P("section", WIDE, NARROW),
        P("section", WIDE, NARROW),
        P("section", WIDE_NARROW, None),
        P("section", WIDE_NARROW, None),
    )
    in_specs = (
        P("section", NARROW, None, WIDE, None),
        P("section", NARROW, None, WIDE, None),
        P("section", NARROW, None, None, WIDE),
        P("section", NARROW, None, WIDE, None),
        P("section", NARROW, None, WIDE),
        P("section", NARROW, None),
    ) + specs
    return jax.shard_map(
        on_device, mesh=finer, in_specs=in_specs, out_specs=specs, check_vma=False
    )
```

```python
import math

import jax
import jax.numpy as jnp
from jax import lax
from jax.experimental import pallas as pl
from jax.experimental.pallas import tpu as pltpu
from jax.sharding import Mesh
from jax.sharding import PartitionSpec as P

D = 4096
FF = 7168
KV = 1024
SECTIONS = 4
ENTRY_COUNT = SECTIONS * (FF * D + D * KV)
AXES = ("section", "wide_0", "wide_1", "narrow_0", "narrow_1")
WIDE = ("wide_0", "wide_1")
NARROW = ("narrow_0", "narrow_1")
WIDE_NARROW = ("wide_0", "wide_1", "narrow_0", "narrow_1")
MESH = pl.DeviceIdType.MESH

MOMENTUM_DECAY = 0.9
STEP_RATE = 0.01

PIECES = ((0, 0), (1, 0), (2, 0), (2, 1), (3, 0), (3, 1), (0, 1), (1, 1))
BY_Z1 = (0, 2, 4, 6)
BY_Z3 = (1, 3, 5, 7)


def flip(value, mask):
    if mask == 0:
        return value
    if mask == 1:
        return value + 1 - 2 * (value % 2)
    if mask == 2:
        return (value + 2) % 4
    return 3 - value


def kernel(
    counts, gates, inputs, value_cot, hidden, cotangent,
    expert_out, value_out, factor_out,
    count_ref, gate_ref, staged, gathered, relay, weights, tokens, token_cots, parts, halves, quarters, cross, eighths, last,
    norms,
    local_sem, token_send, token_recv, cot_send, cot_recv, z_send, z_recv, zf_send, zf_recv,
    hid_send, hid_recv, val_send, val_recv, norm_send, norm_recv,
):
    section = lax.axis_index("section")
    z = lax.axis_index("wide_0")
    hi = lax.axis_index("wide_1")
    lo = lax.axis_index("narrow_0")
    core = lax.axis_index("narrow_1")
    x = 2 * hi + lo
    side = (hi, 1 - hi)

    def device(dy=0, dz=0, dx=0, dc=0):
        there = flip(x, dx)
        return (flip(section, dy), flip(z, dz), there // 2, there % 2, 1 - core if dc else core)

    def send(src, dst, send_sem, recv_sem, **where):
        return pltpu.make_async_remote_copy(
            src_ref=src, dst_ref=dst, send_sem=send_sem, recv_sem=recv_sem,
            device_id=device(**where), device_id_type=MESH,
        )

    pending = []

    def start(copy):
        copy.start()
        pending.append(copy)
        return copy

    peers = [dict(dx=i // 2, dc=i % 2) for i in range(1, 8)]
    peers += [dict(dz=i % 4, dy=i // 4) for i in range(1, 16)]

    barrier = pltpu.get_barrier_semaphore()
    for peer in peers:
        pl.semaphore_signal(barrier, inc=1, device_id=device(**peer), device_id_type=MESH)

    small_loads = [
        pltpu.make_async_copy(counts, count_ref, local_sem.at[10]),
        pltpu.make_async_copy(gates, gate_ref, local_sem.at[11]),
    ]
    for load in small_loads:
        load.start()
    cot_loads = []
    for rel in range(4):
        column = (2 * (1 - lo if rel // 2 else lo) + (1 - core if rel % 2 else core)) * 1024
        source = cotangent.at[:, :, pl.ds(pl.multiple_of(column, 1024), 1024)]
        load = pltpu.make_async_copy(source, staged.at[rel], local_sem.at[rel])
        load.start()
        cot_loads.append(load)
    load_cots = pltpu.make_async_copy(value_cot, token_cots.at[0], local_sem.at[4])
    load_cots.start()
    others = []
    for dx in range(4):
        for dz in range(4):
            block = 2 * (4 * flip(z, dz) + flip(x, dx))
            place = pl.ds((dx * 4 + dz) * 128, 128)
            for which, owner in ((0, core), (1, 1 - core)):
                source = inputs.at[:, pl.ds(pl.multiple_of((block + owner) * 128, 128), 128)]
                if which == 0:
                    pltpu.make_async_copy(source, tokens.at[0, :, place], local_sem.at[5]).start()
                else:
                    others.append((source, place))
    hid_loads = []
    for dz in range(4):
        rows = pl.ds(pl.multiple_of(flip(z, dz) * 64, 64), 64)
        load = pltpu.make_async_copy(hidden.at[:, rows, :], weights.at[0, dz], local_sem.at[6 + dz])
        load.start()
        hid_loads.append(load)

    lanes = lax.broadcasted_iota(jnp.int32, (1, 32), 1) + (2 * z + hi) * 32
    diagonal = lax.broadcasted_iota(jnp.int32, (32, 32), 0) == lax.broadcasted_iota(
        jnp.int32, (32, 32), 1
    )
    columns = []
    for load in small_loads:
        load.wait()
    for micro in range(4):
        gate = gate_ref[micro : micro + 1, :].astype(jnp.float32)
        row = jnp.where(lanes < count_ref[micro], gate, jnp.zeros_like(gate))
        square = jnp.where(diagonal, jnp.broadcast_to(row, (32, 32)), 0.0)
        columns.append(jnp.sum(square, axis=1, keepdims=True))

    def scale(rel):
        cot_loads[rel].wait()
        for micro in range(4):
            scaled = (columns[micro] * staged[rel, micro].astype(jnp.float32)).astype(jnp.bfloat16)
            if rel == 0:
                gathered[0, 0, micro, hi] = scaled
            else:
                staged[rel, micro] = scaled

    def piece(slot, index):
        replica, far = PIECES[index]
        return gathered.at[slot, replica, :, side[far]]

    def along_z(index):
        start(send(piece(0, index), piece(1, index), z_send.at[0, index], z_recv.at[0, index], dz=1))
        start(send(piece(0, index), piece(3, index), z_send.at[1, index], z_recv.at[1, index], dz=3))

    def z_arrival(link, index):
        slot = (1, 3)[link]
        return send(piece(0, index), piece(slot, index), z_send.at[link, index], z_recv.at[link, index], dz=slot)

    def forward_z(index):
        if index in BY_Z1:
            z_arrival(1, index).wait_recv()
            start(send(piece(3, index), piece(2, index), zf_send.at[index], zf_recv.at[index], dz=1))
        else:
            z_arrival(0, index).wait_recv()
            start(send(piece(1, index), piece(2, index), zf_send.at[index], zf_recv.at[index], dz=3))

    def into(replica, far):
        return gathered.at[0, replica, :, side[far]]

    mine_0 = into(0, 0)
    cot = {}

    def cot_send_of(name, index, src, dst, **where):
        cot[name] = start(send(src, dst, cot_send.at[index], cot_recv.at[index], **where))

    scale(0)
    scale(1)
    pl.semaphore_wait(barrier, len(peers))
    along_z(0)
    cot_send_of("relay_1", 1, mine_0, relay.at[0], dx=1)
    cot_send_of("relay_3", 2, staged.at[1], relay.at[1], dx=3)
    cot_send_of("core", 0, staged.at[1], into(1, 0), dc=1)
    scale(2)
    scale(3)
    cot_send_of("x1_same", 3, staged.at[2], into(2, 0), dx=1)
    cot_send_of("x3_same", 4, staged.at[2], into(2, 0), dx=3)
    cot_send_of("x1_cross", 5, staged.at[3], into(3, 0), dx=1, dc=1)
    cot_send_of("x3_cross", 6, staged.at[3], into(3, 0), dx=3, dc=1)

    for source, place in others:
        send(source, tokens.at[1, :, place], token_send.at[0], token_recv.at[0], dc=1).start()
    token_whole = send(tokens.at[1], tokens.at[1], token_send.at[0], token_recv.at[0], dc=1)
    pending.append(token_whole)
    cots_whole = start(send(value_cot, token_cots.at[1], token_send.at[1], token_recv.at[1], dc=1))
    hid_core = []
    for dz in range(4):
        rows = pl.ds(pl.multiple_of(flip(z, dz) * 64, 64), 64)
        hid_core.append(
            start(send(hidden.at[:, rows, :], weights.at[1, dz], hid_send.at[0, dz], hid_recv.at[0, dz], dc=1))
        )

    cot["core"].wait_recv()
    along_z(1)

    load_cots.wait()
    pltpu.make_async_copy(tokens.at[0], tokens.at[0], local_sem.at[5]).wait()
    token_whole.wait_recv()
    cots_whole.wait_recv()

    def value_parts(dx):
        def block(dz, carry):
            place = pl.ds(pl.multiple_of((dx * 4 + dz) * 128, 128), 128)
            lhs = tokens[:, :, place].reshape(768, 128)
            rhs = token_cots[...].reshape(768, KV)
            product = lax.dot_general(
                lhs, rhs, (((0,), (0,)), ((), ())), preferred_element_type=jnp.float32
            )
            parts[dx, dz] = product.astype(jnp.bfloat16)
            return carry

        lax.fori_loop(0, 4, block, 0)

    value = {}

    def value_send(name, index, src, dst, **where):
        value[name] = start(send(src, dst, val_send.at[index], val_recv.at[index], **where))

    hid_far = {}

    def send_hidden(dz):
        hid_loads[dz].wait()
        hid_far[dz] = start(
            send(weights.at[0, dz], weights.at[2, dz], hid_send.at[1, dz], hid_recv.at[1, dz], dx=1)
        )

    value_parts(2)
    cot["relay_1"].wait_recv()
    cot_send_of("far_3", 7, relay.at[0], into(0, 0), dx=3)
    cot["relay_3"].wait_recv()
    cot_send_of("far_1", 8, relay.at[1], into(1, 1), dx=1, dc=1)
    for dz in (0, 1, 3):
        send_hidden(dz)
    value_parts(3)
    for i, (far, dz) in enumerate(((1, 2), (0, 2), (1, 1), (1, 3), (1, 0), (0, 3), (0, 1), (0, 0))):
        value_send(("x3", far, dz), i, parts.at[3 - far, dz], halves.at[far, dz], dx=3)
    cot["x1_same"].wait_recv()
    along_z(2)
    cot["x3_same"].wait_recv()
    along_z(3)
    value_parts(1)
    cot["x1_cross"].wait_recv()
    along_z(4)
    cot["x3_cross"].wait_recv()
    along_z(5)
    value_parts(0)
    cot["far_3"].wait_recv()
    along_z(6)
    cot["far_1"].wait_recv()
    along_z(7)

    def products(slot, replica, first=False):
        def tile(n, carry):
            place = pl.ds(pl.multiple_of(n * 256, 256), 256)
            lhs = weights[replica, slot].reshape(256, 896)
            rhs = gathered[slot, replica, :, :, :, place].reshape(256, 256)
            product = lax.dot_general(
                lhs, rhs, (((0,), (0,)), ((), ())), preferred_element_type=jnp.float32
            )
            if first:
                expert_out[:, place] = product
            else:
                expert_out[:, place] += product
            return carry

        lax.fori_loop(0, 4, tile, 0)

    def second_step(dz, more=None):
        value[("x3", 1, dz)].wait_recv()
        total = parts[1, dz].astype(jnp.float32) + halves[1, dz].astype(jnp.float32)
        if more is not None:
            total = total + more[...].astype(jnp.float32)
        parts[1, dz] = total.astype(jnp.bfloat16)

    def second_send(dz):
        value_send(("x1", dz), 8 + dz, parts.at[1, dz], quarters.at[dz], dx=1)

    hid_pass = {}

    def pass_hidden(dz):
        hid_far[dz].wait_recv()
        hid_pass[dz] = start(
            send(weights.at[2, dz], weights.at[3, dz], hid_send.at[2, dz], hid_recv.at[2, dz], dc=1)
        )

    def far_arrival(index):
        if index in BY_Z1:
            send(piece(3, index), piece(2, index), zf_send.at[index], zf_recv.at[index], dz=1).wait_recv()
        else:
            send(piece(1, index), piece(2, index), zf_send.at[index], zf_recv.at[index], dz=3).wait_recv()

    def third_step(dz):
        value[("x3", 0, dz)].wait_recv()
        total = parts[0, dz].astype(jnp.float32) + halves[0, dz].astype(jnp.float32)
        if dz != 2:
            value[("x1", dz)].wait_recv()
            total = total + quarters[dz].astype(jnp.float32)
        return total

    products(0, 0, first=True)
    second_step(2)
    hid_core[0].wait_recv()
    products(0, 1)
    value_send("cross", 10, parts.at[1, 2], cross, dz=3)
    parts[0, 2] = third_step(2).astype(jnp.bfloat16)
    forward_z(0)
    forward_z(1)
    value_send("z1_1", 13, parts.at[0, 2], eighths.at[1], dz=1)
    forward_z(2)
    forward_z(3)
    forward_z(4)
    pass_hidden(0)
    products(0, 2)
    forward_z(5)
    hid_pass[0].wait_recv()
    products(0, 3)
    forward_z(6)
    pass_hidden(1)
    second_step(3)
    forward_z(7)
    second_send(3)
    z_arrival(0, 0).wait_recv()
    z_arrival(0, 6).wait_recv()
    products(1, 0)
    second_step(0)
    value["cross"].wait_recv()
    second_step(1, cross)
    hid_core[1].wait_recv()
    z_arrival(1, 1).wait_recv()
    z_arrival(1, 7).wait_recv()
    products(1, 1)
    second_send(1)
    send_hidden(2)
    second_send(0)
    z_arrival(0, 2).wait_recv()
    products(1, 2)
    pass_hidden(3)
    hid_pass[1].wait_recv()
    z_arrival(0, 4).wait_recv()
    products(1, 3)
    third = third_step(3)
    value["z1_1"].wait_recv()
    parts[0, 3] = (third + eighths[1].astype(jnp.float32)).astype(jnp.bfloat16)
    products(3, 0)
    value_send("z3", 14, parts.at[0, 3], last, dz=3)
    parts[0, 1] = third_step(1).astype(jnp.bfloat16)
    hid_core[3].wait_recv()
    products(3, 1)
    value_send("z1_0", 12, parts.at[0, 1], eighths.at[0], dz=1)
    z_arrival(1, 3).wait_recv()
    products(3, 2)
    hid_pass[3].wait_recv()
    z_arrival(1, 5).wait_recv()
    products(3, 3)
    pass_hidden(2)
    far_arrival(2)
    far_arrival(3)
    products(2, 2)
    far_arrival(4)
    far_arrival(5)
    hid_pass[2].wait_recv()
    products(2, 3)
    far_arrival(0)
    far_arrival(6)
    products(2, 0)
    hid_core[2].wait_recv()
    far_arrival(1)
    far_arrival(7)
    products(2, 1)

    def squares(ref, rows):
        def tile(i, total):
            chunk = ref[pl.ds(pl.multiple_of(i * 8, 8), 8), :]
            for n in range(8):
                one = chunk[:, n * 128 : (n + 1) * 128]
                total = total + one * one
            return total

        return lax.fori_loop(0, rows // 8, tile, jnp.zeros((8, 128), jnp.float32))

    expert_squares = squares(expert_out, 896)
    near = third_step(0)
    value["z1_0"].wait_recv()
    near = near + eighths[0].astype(jnp.float32)
    value["z3"].wait_recv()
    value_out[...] = near + last[...].astype(jnp.float32)
    norms[0] = expert_squares + squares(value_out, 128)

    base = 0
    slot = 1
    for group in (peers[:7], peers[7:]):
        copies = []
        for i, peer in enumerate(group):
            copies.append(
                start(
                    send(norms.at[base], norms.at[slot + i], norm_send.at[slot + i], norm_recv.at[slot + i], **peer)
                )
            )
        total = norms[base]
        for i, copy in enumerate(copies):
            copy.wait_recv()
            total = total + norms[slot + i]
        base = slot + len(group)
        norms[base] = total
        slot = base + 1
    overall = jnp.sum(jnp.sum(norms[base], axis=0, keepdims=True), axis=1, keepdims=True)
    overall = jnp.broadcast_to(overall, (8, 128))
    factor_out[...] = jnp.minimum(1.0, math.sqrt(ENTRY_COUNT) / jnp.sqrt(overall + 1e-06))

    for copy in pending:
        copy.wait_send()


def update_kernel(
    factor_ref, expert_grad, expert_moment, expert_weight, value_grad, value_moment, value_weight,
    expert_weight_out, expert_moment_out, value_weight_out, value_moment_out,
    new_weights, new_moments, weight_sem, moment_sem,
):
    factor = factor_ref[0:1, 0:1]
    copies = []
    for tile in range(8):
        rows = pl.ds(tile * 128, 128)
        if tile < 7:
            there, refs = rows, (expert_grad, expert_moment, expert_weight)
            outs = (expert_weight_out, expert_moment_out)
        else:
            there, refs = pl.ds(0, 128), (value_grad, value_moment, value_weight)
            outs = (value_weight_out, value_moment_out)

        def chunk(i, carry, tile=tile, refs=refs):
            grad, moment, weight = refs
            at = pl.ds(pl.multiple_of((tile % 7) * 128 + i * 16, 16), 16)
            to = pl.ds(pl.multiple_of(tile * 128 + i * 16, 16), 16)
            moved = MOMENTUM_DECAY * moment[at, :] + factor * grad[at, :]
            new_moments[to, :] = moved
            new_weights[to, :] = (weight[at, :].astype(jnp.float32) - STEP_RATE * moved).astype(
                jnp.bfloat16
            )
            return carry

        lax.fori_loop(0, 8, chunk, 0)
        for src, dst, sem in (
            (new_weights, outs[0], weight_sem),
            (new_moments, outs[1], moment_sem),
        ):
            copy = pltpu.make_async_copy(src.at[rows, :], dst.at[there, :], sem.at[tile])
            copy.start()
            copies.append(copy)
    for copy in copies:
        copy.wait()


def on_device(
    normed_inputs, value_cotangent, expert_hidden, expert_cotangent, slot_gate, slot_count,
    expert_weight, expert_moment, value_weight, value_moment,
):
    bf16 = jnp.bfloat16
    in_hbm = pl.BlockSpec(memory_space=pltpu.HBM)
    vmem = pl.BlockSpec(memory_space=pltpu.VMEM)
    dma = pltpu.SemaphoreType.DMA
    expert_grad, value_grad, factor = pl.pallas_call(
        kernel,
        name="gradients",
        out_shape=(
            pltpu.VMEM((896, 1024), jnp.float32),
            pltpu.VMEM((128, 1024), jnp.float32),
            pltpu.VMEM((8, 128), jnp.float32),
        ),
        in_specs=[in_hbm] * 6,
        out_specs=(vmem, vmem, vmem),
        scratch_shapes=[
            pltpu.SMEM((4,), jnp.int32),
            pltpu.VMEM((4, 32), bf16),
            pltpu.VMEM((4, 4, 32, 1024), bf16),
            pltpu.VMEM((4, 4, 4, 2, 32, 1024), bf16),
            pltpu.VMEM((2, 4, 32, 1024), bf16),
            pltpu.VMEM((4, 4, 4, 64, 896), bf16),
            pltpu.VMEM((2, 384, 2048), bf16),
            pltpu.VMEM((2, 384, 1024), bf16),
            pltpu.VMEM((4, 4, 128, 1024), bf16),
            pltpu.VMEM((2, 4, 128, 1024), bf16),
            pltpu.VMEM((4, 128, 1024), bf16),
            pltpu.VMEM((128, 1024), bf16),
            pltpu.VMEM((2, 128, 1024), bf16),
            pltpu.VMEM((128, 1024), bf16),
            pltpu.VMEM((25, 8, 128), jnp.float32),
            dma((12,)),
            dma((2,)), dma((2,)),
            dma((9,)), dma((9,)),
            dma((2, 8)), dma((2, 8)),
            dma((8,)), dma((8,)),
            dma((3, 4)), dma((3, 4)),
            dma((15,)), dma((15,)),
            dma((24,)), dma((24,)),
        ],
        compiler_params=pltpu.CompilerParams(
            collective_id=0, has_side_effects=True, vmem_limit_bytes=46 * 1024 * 1024
        ),
        cost_estimate=pl.CostEstimate(
            flops=2 * 896 * 1024 * 4096 + 2 * 2048 * 1024 * 768,
            bytes_accessed=10_000_000,
            transcendentals=0,
        ),
    )(
        pltpu.with_memory_space_constraint(slot_count[0, 0], pltpu.HBM),
        pltpu.with_memory_space_constraint(slot_gate[0, 0], pltpu.HBM),
        pltpu.with_memory_space_constraint(normed_inputs[0, 0].reshape(384, D), pltpu.HBM),
        pltpu.with_memory_space_constraint(value_cotangent[0, 0].reshape(384, KV), pltpu.HBM),
        pltpu.with_memory_space_constraint(expert_hidden[0, 0], pltpu.HBM),
        pltpu.with_memory_space_constraint(expert_cotangent[0, 0], pltpu.HBM),
    )
    expert_weight_next, expert_next, value_weight_next, value_next = pl.pallas_call(
        update_kernel,
        name="update",
        out_shape=(
            jax.ShapeDtypeStruct((896, 1024), bf16),
            jax.ShapeDtypeStruct((896, 1024), jnp.float32),
            jax.ShapeDtypeStruct((128, 1024), bf16),
            jax.ShapeDtypeStruct((128, 1024), jnp.float32),
        ),
        in_specs=[vmem] * 7,
        out_specs=(in_hbm,) * 4,
        scratch_shapes=[
            pltpu.VMEM((1024, 1024), bf16),
            pltpu.VMEM((1024, 1024), jnp.float32),
            dma((8,)),
            dma((8,)),
        ],
        compiler_params=pltpu.CompilerParams(vmem_limit_bytes=24 * 1024 * 1024),
        cost_estimate=pl.CostEstimate(flops=6 * 1024 * 1024, bytes_accessed=6_000_000, transcendentals=0),
    )(
        factor, expert_grad, expert_moment[0], expert_weight[0],
        value_grad, value_moment[0], value_weight[0],
    )
    return (expert_weight_next[None], expert_next[None], value_weight_next[None], value_next[None])


def solution(mesh):
    finer = Mesh(mesh.devices.reshape(mesh.shape["section"], 4, 2, 2, 2), AXES)
    specs = (
        P("section", WIDE, NARROW),
        P("section", WIDE, NARROW),
        P("section", WIDE_NARROW, None),
        P("section", WIDE_NARROW, None),
    )
    in_specs = (
        P("section", NARROW, None, WIDE, None),
        P("section", NARROW, None, WIDE, None),
        P("section", NARROW, None, None, WIDE),
        P("section", NARROW, None, WIDE, None),
        P("section", NARROW, None, WIDE),
        P("section", NARROW, None),
    ) + specs
    return jax.shard_map(
        on_device, mesh=finer, in_specs=in_specs, out_specs=specs, check_vma=False
    )
```

```python
import math

import jax
import jax.numpy as jnp
from jax import lax
from jax.experimental import pallas as pl
from jax.experimental.pallas import tpu as pltpu
from jax.sharding import Mesh
from jax.sharding import PartitionSpec as P

D = 4096
FF = 7168
KV = 1024
SECTIONS = 4
ENTRY_COUNT = SECTIONS * (FF * D + D * KV)
AXES = ("section", "wide_0", "wide_1", "narrow_0", "narrow_1")
WIDE = ("wide_0", "wide_1")
NARROW = ("narrow_0", "narrow_1")
WIDE_NARROW = ("wide_0", "wide_1", "narrow_0", "narrow_1")
MESH = pl.DeviceIdType.MESH

MOMENTUM_DECAY = 0.9
STEP_RATE = 0.01

PIECES = ((0, 0), (1, 0), (2, 0), (2, 1), (3, 0), (3, 1), (0, 1), (1, 1))
BY_Z1 = (0, 2, 4, 6)
BY_Z3 = (1, 3, 5, 7)


def flip(value, mask):
    if mask == 0:
        return value
    if mask == 1:
        return value + 1 - 2 * (value % 2)
    if mask == 2:
        return (value + 2) % 4
    return 3 - value


def kernel(
    counts, gates, inputs, value_cot, hidden, cotangent,
    expert_moment, expert_weight, value_moment, value_weight,
    grads_out, moments_out, weights_out, factor_out,
    count_ref, gate_ref, staged, gathered, relay, weights, tokens, token_cots, parts, halves, quarters, cross, eighths, last,
    norms,
    local_sem, token_send, token_recv, cot_send, cot_recv, z_send, z_recv, zf_send, zf_recv,
    hid_send, hid_recv, val_send, val_recv, norm_send, norm_recv,
):
    section = lax.axis_index("section")
    z = lax.axis_index("wide_0")
    hi = lax.axis_index("wide_1")
    lo = lax.axis_index("narrow_0")
    core = lax.axis_index("narrow_1")
    x = 2 * hi + lo
    side = (hi, 1 - hi)

    def device(dy=0, dz=0, dx=0, dc=0):
        there = flip(x, dx)
        return (flip(section, dy), flip(z, dz), there // 2, there % 2, 1 - core if dc else core)

    def send(src, dst, send_sem, recv_sem, **where):
        return pltpu.make_async_remote_copy(
            src_ref=src, dst_ref=dst, send_sem=send_sem, recv_sem=recv_sem,
            device_id=device(**where), device_id_type=MESH,
        )

    pending = []

    def start(copy):
        copy.start()
        pending.append(copy)
        return copy

    peers = [dict(dx=i // 2, dc=i % 2) for i in range(1, 8)]
    peers += [dict(dz=i % 4, dy=i // 4) for i in range(1, 16)]

    barrier = pltpu.get_barrier_semaphore()
    for peer in peers:
        pl.semaphore_signal(barrier, inc=1, device_id=device(**peer), device_id_type=MESH)

    small_loads = [
        pltpu.make_async_copy(counts, count_ref, local_sem.at[10]),
        pltpu.make_async_copy(gates, gate_ref, local_sem.at[11]),
    ]
    for load in small_loads:
        load.start()
    cot_loads = []
    for rel in range(4):
        column = (2 * (1 - lo if rel // 2 else lo) + (1 - core if rel % 2 else core)) * 1024
        source = cotangent.at[:, :, pl.ds(pl.multiple_of(column, 1024), 1024)]
        load = pltpu.make_async_copy(source, staged.at[rel], local_sem.at[rel])
        load.start()
        cot_loads.append(load)
    lanes = lax.broadcasted_iota(jnp.int32, (1, 32), 1) + (2 * z + hi) * 32
    diagonal = lax.broadcasted_iota(jnp.int32, (32, 32), 0) == lax.broadcasted_iota(
        jnp.int32, (32, 32), 1
    )
    columns = []
    for load in small_loads:
        load.wait()
    for micro in range(4):
        gate = gate_ref[micro : micro + 1, :].astype(jnp.float32)
        row = jnp.where(lanes < count_ref[micro], gate, jnp.zeros_like(gate))
        square = jnp.where(diagonal, jnp.broadcast_to(row, (32, 32)), 0.0)
        columns.append(jnp.sum(square, axis=1, keepdims=True))

    def scale(rel):
        cot_loads[rel].wait()
        for micro in range(4):
            scaled = (columns[micro] * staged[rel, micro].astype(jnp.float32)).astype(jnp.bfloat16)
            if rel == 0:
                gathered[0, 0, micro, hi] = scaled
            else:
                staged[rel, micro] = scaled

    def piece(slot, index):
        replica, far = PIECES[index]
        return gathered.at[slot, replica, :, side[far]]

    def along_z(index):
        start(send(piece(0, index), piece(1, index), z_send.at[0, index], z_recv.at[0, index], dz=1))
        start(send(piece(0, index), piece(3, index), z_send.at[1, index], z_recv.at[1, index], dz=3))

    def z_arrival(link, index):
        slot = (1, 3)[link]
        return send(piece(0, index), piece(slot, index), z_send.at[link, index], z_recv.at[link, index], dz=slot)

    def forward_z(index):
        if index in BY_Z1:
            z_arrival(1, index).wait_recv()
            start(send(piece(3, index), piece(2, index), zf_send.at[index], zf_recv.at[index], dz=1))
        else:
            z_arrival(0, index).wait_recv()
            start(send(piece(1, index), piece(2, index), zf_send.at[index], zf_recv.at[index], dz=3))

    def into(replica, far):
        return gathered.at[0, replica, :, side[far]]

    mine_0 = into(0, 0)
    cot = {}

    def cot_send_of(name, index, src, dst, **where):
        cot[name] = start(send(src, dst, cot_send.at[index], cot_recv.at[index], **where))

    scale(0)
    scale(2)
    pl.semaphore_wait(barrier, len(peers))
    along_z(0)
    scale(1)
    cot_send_of("x1_same", 3, staged.at[2], into(2, 0), dx=1)
    cot_send_of("x3_same", 4, staged.at[2], into(2, 0), dx=3)
    cot_send_of("relay_1", 1, mine_0, relay.at[0], dx=1)
    scale(3)
    cot_send_of("core", 0, staged.at[1], into(1, 0), dc=1)
    cot_send_of("relay_3", 2, staged.at[1], relay.at[1], dx=3)
    cot_send_of("x1_cross", 5, staged.at[3], into(3, 0), dx=1, dc=1)
    cot_send_of("x3_cross", 6, staged.at[3], into(3, 0), dx=3, dc=1)

    load_cots = pltpu.make_async_copy(value_cot, token_cots.at[0], local_sem.at[4])
    load_cots.start()
    others = []
    for dx in range(4):
        for dz in range(4):
            block = 2 * (4 * flip(z, dz) + flip(x, dx))
            place = pl.ds((dx * 4 + dz) * 128, 128)
            for which, owner in ((0, core), (1, 1 - core)):
                source = inputs.at[:, pl.ds(pl.multiple_of((block + owner) * 128, 128), 128)]
                if which == 0:
                    pltpu.make_async_copy(source, tokens.at[0, :, place], local_sem.at[5]).start()
                else:
                    others.append((source, place))
    hid_loads = []
    for dz in range(4):
        rows = pl.ds(2 * flip(z, dz), 2)
        load = pltpu.make_async_copy(hidden.at[:, rows], weights.at[0, dz], local_sem.at[6 + dz])
        load.start()
        hid_loads.append(load)
    state_loads = [
        pltpu.make_async_copy(expert_moment, moments_out.at[0:896], local_sem.at[12]),
        pltpu.make_async_copy(expert_weight, weights_out.at[0:896], local_sem.at[13]),
        pltpu.make_async_copy(value_moment, moments_out.at[896:1024], local_sem.at[14]),
        pltpu.make_async_copy(value_weight, weights_out.at[896:1024], local_sem.at[15]),
    ]

    for source, place in others:
        send(source, tokens.at[1, :, place], token_send.at[0], token_recv.at[0], dc=1).start()
    token_whole = send(tokens.at[1], tokens.at[1], token_send.at[0], token_recv.at[0], dc=1)
    pending.append(token_whole)
    cots_whole = start(send(value_cot, token_cots.at[1], token_send.at[1], token_recv.at[1], dc=1))
    hid_core = []
    for dz in range(4):
        rows = pl.ds(2 * flip(z, dz), 2)
        hid_core.append(
            start(send(hidden.at[:, rows], weights.at[1, dz], hid_send.at[0, dz], hid_recv.at[0, dz], dc=1))
        )

    cot["core"].wait_recv()
    along_z(1)

    load_cots.wait()
    pltpu.make_async_copy(tokens.at[0], tokens.at[0], local_sem.at[5]).wait()
    token_whole.wait_recv()
    cots_whole.wait_recv()

    def value_parts(dx):
        def block(dz, carry):
            place = pl.ds(pl.multiple_of((dx * 4 + dz) * 128, 128), 128)
            lhs = tokens[:, :, place].reshape(768, 128)
            rhs = token_cots[...].reshape(768, KV)
            product = lax.dot_general(
                lhs, rhs, (((0,), (0,)), ((), ())), preferred_element_type=jnp.float32
            )
            parts[dx, dz] = product.astype(jnp.bfloat16)
            return carry

        lax.fori_loop(0, 4, block, 0)

    value = {}

    def value_send(name, index, src, dst, **where):
        value[name] = start(send(src, dst, val_send.at[index], val_recv.at[index], **where))

    hid_far = {}

    def send_hidden(dz):
        hid_loads[dz].wait()
        hid_far[dz] = start(
            send(weights.at[0, dz], weights.at[2, dz], hid_send.at[1, dz], hid_recv.at[1, dz], dx=1)
        )

    value_parts(2)
    cot["x1_same"].wait_recv()
    along_z(2)
    cot["x3_same"].wait_recv()
    along_z(3)
    value_parts(3)
    cot["relay_1"].wait_recv()
    cot_send_of("far_3", 7, relay.at[0], into(0, 0), dx=3)
    cot["relay_3"].wait_recv()
    cot_send_of("far_1", 8, relay.at[1], into(1, 1), dx=1, dc=1)
    for dz in (0, 1, 3):
        send_hidden(dz)
    for i, (far, dz) in enumerate(((1, 2), (0, 2), (1, 1), (1, 3), (1, 0), (0, 3), (0, 1), (0, 0))):
        value_send(("x3", far, dz), i, parts.at[3 - far, dz], halves.at[far, dz], dx=3)
    for load in state_loads:
        load.start()
    value_parts(1)
    cot["x1_cross"].wait_recv()
    along_z(4)
    cot["x3_cross"].wait_recv()
    along_z(5)
    value_parts(0)
    cot["far_3"].wait_recv()
    along_z(6)
    cot["far_1"].wait_recv()
    along_z(7)

    def accumulate(weights_of, gathered_of, first=False):
        def tile(n, carry):
            place = pl.ds(pl.multiple_of(n * 256, 256), 256)
            lhs = weights_of().reshape(256, 896)
            rhs = gathered_of(place).reshape(256, 256)
            product = lax.dot_general(
                lhs, rhs, (((0,), (0,)), ((), ())), preferred_element_type=jnp.float32
            )
            if first:
                grads_out[0:896, place] = product
            else:
                grads_out[0:896, place] += product
            return carry

        lax.fori_loop(0, 4, tile, 0)

    def products(slot, replica, first=False):
        accumulate(
            lambda: weights[replica, slot],
            lambda place: gathered[slot, replica, :, :, :, place],
            first,
        )

    def chip_products(slot, far):
        accumulate(
            lambda: weights[0:2, slot, :, side[far]],
            lambda place: gathered[slot, 0:2, :, side[far], :, place],
        )

    def second_step(dz, more=None):
        value[("x3", 1, dz)].wait_recv()
        total = parts[1, dz].astype(jnp.float32) + halves[1, dz].astype(jnp.float32)
        if more is not None:
            total = total + more[...].astype(jnp.float32)
        parts[1, dz] = total.astype(jnp.bfloat16)

    def second_send(dz):
        value_send(("x1", dz), 8 + dz, parts.at[1, dz], quarters.at[dz], dx=1)

    hid_pass = {}

    def pass_hidden(dz):
        hid_far[dz].wait_recv()
        hid_pass[dz] = start(
            send(weights.at[2, dz], weights.at[3, dz], hid_send.at[2, dz], hid_recv.at[2, dz], dc=1)
        )

    def far_arrival(index):
        if index in BY_Z1:
            send(piece(3, index), piece(2, index), zf_send.at[index], zf_recv.at[index], dz=1).wait_recv()
        else:
            send(piece(1, index), piece(2, index), zf_send.at[index], zf_recv.at[index], dz=3).wait_recv()

    def third_step(dz):
        value[("x3", 0, dz)].wait_recv()
        total = parts[0, dz].astype(jnp.float32) + halves[0, dz].astype(jnp.float32)
        if dz != 2:
            value[("x1", dz)].wait_recv()
            total = total + quarters[dz].astype(jnp.float32)
        return total

    products(0, 0, first=True)
    second_step(2)
    hid_core[0].wait_recv()
    products(0, 1)
    value_send("cross", 10, parts.at[1, 2], cross, dz=3)
    parts[0, 2] = third_step(2).astype(jnp.bfloat16)
    forward_z(0)
    forward_z(1)
    value_send("z1_1", 13, parts.at[0, 2], eighths.at[1], dz=1)
    forward_z(2)
    forward_z(3)
    forward_z(4)
    pass_hidden(0)
    products(0, 2)
    forward_z(5)
    hid_pass[0].wait_recv()
    products(0, 3)
    forward_z(6)
    pass_hidden(1)
    second_step(3)
    forward_z(7)
    second_send(3)
    z_arrival(0, 0).wait_recv()
    z_arrival(0, 6).wait_recv()
    products(1, 0)
    second_step(0)
    value["cross"].wait_recv()
    second_step(1, cross)
    hid_core[1].wait_recv()
    z_arrival(1, 1).wait_recv()
    z_arrival(1, 7).wait_recv()
    products(1, 1)
    second_send(1)
    send_hidden(2)
    second_send(0)
    z_arrival(0, 2).wait_recv()
    products(1, 2)
    pass_hidden(3)
    hid_pass[1].wait_recv()
    z_arrival(0, 4).wait_recv()
    products(1, 3)
    third = third_step(3)
    value["z1_1"].wait_recv()
    parts[0, 3] = (third + eighths[1].astype(jnp.float32)).astype(jnp.bfloat16)
    products(3, 0)
    value_send("z3", 14, parts.at[0, 3], last, dz=3)
    parts[0, 1] = third_step(1).astype(jnp.bfloat16)
    hid_core[3].wait_recv()
    products(3, 1)
    value_send("z1_0", 12, parts.at[0, 1], eighths.at[0], dz=1)
    z_arrival(1, 3).wait_recv()
    products(3, 2)
    hid_pass[3].wait_recv()
    z_arrival(1, 5).wait_recv()
    products(3, 3)
    hid_core[2].wait_recv()
    far_arrival(0)
    far_arrival(1)
    chip_products(2, 0)
    pass_hidden(2)
    far_arrival(2)
    far_arrival(3)
    products(2, 2)
    hid_pass[2].wait_recv()
    far_arrival(4)
    far_arrival(5)
    products(2, 3)
    far_arrival(6)
    far_arrival(7)
    chip_products(2, 1)

    def squares(first, rows):
        def tile(i, totals):
            chunk = grads_out[pl.ds(pl.multiple_of(first + i * 32, 32), 32), :]
            totals = list(totals)
            for group in range(4):
                for n in range(8):
                    one = chunk[group * 8 : (group + 1) * 8, n * 128 : (n + 1) * 128]
                    totals[n] = totals[n] + one * one
            return tuple(totals)

        totals = lax.fori_loop(0, rows // 32, tile, (jnp.zeros((8, 128), jnp.float32),) * 8)
        return sum(totals[1:], totals[0])

    expert_squares = squares(0, 896)
    for load in state_loads:
        load.wait()
    near = third_step(0)
    value["z1_0"].wait_recv()
    near = near + eighths[0].astype(jnp.float32)
    value["z3"].wait_recv()
    grads_out[896:1024, :] = near + last[...].astype(jnp.float32)
    norms[0] = expert_squares + squares(896, 128)
    started = len(pending)

    base = 0
    slot = 1
    for group in (peers[:7], peers[7:]):
        copies = []
        for i, peer in enumerate(group):
            copies.append(
                start(
                    send(norms.at[base], norms.at[slot + i], norm_send.at[slot + i], norm_recv.at[slot + i], **peer)
                )
            )
        if base == 0:
            for copy in pending[:started]:
                copy.wait_send()
        total = norms[base]
        for i, copy in enumerate(copies):
            copy.wait_recv()
            total = total + norms[slot + i]
        base = slot + len(group)
        norms[base] = total
        slot = base + 1
    overall = jnp.sum(jnp.sum(norms[base], axis=0, keepdims=True), axis=1, keepdims=True)
    overall = jnp.broadcast_to(overall, (8, 128))
    factor_out[...] = jnp.minimum(1.0, math.sqrt(ENTRY_COUNT) / jnp.sqrt(overall + 1e-06))

    for copy in pending[started:]:
        copy.wait_send()


def update_kernel(
    factor_ref, grads, moments, weights,
    expert_weight_out, expert_moment_out, value_weight_out, value_moment_out,
    new_weights, new_moments, weight_sem, moment_sem,
):
    factor = factor_ref[0:1, 0:1]
    copies = []
    for tile in range(8):

        def chunk(i, carry, tile=tile):
            at = pl.ds(pl.multiple_of(tile * 128 + i * 32, 32), 32)
            moved = MOMENTUM_DECAY * moments[at, :] + factor * grads[at, :]
            new_moments[at, :] = moved
            new_weights[at, :] = (weights[at, :].astype(jnp.float32) - STEP_RATE * moved).astype(
                jnp.bfloat16
            )
            return carry

        lax.fori_loop(0, 4, chunk, 0)
        rows = pl.ds(tile * 128, 128)
        there = rows if tile < 7 else pl.ds(0, 128)
        outs = (expert_weight_out, expert_moment_out) if tile < 7 else (value_weight_out, value_moment_out)
        for src, dst, sem in (
            (new_weights, outs[0], weight_sem),
            (new_moments, outs[1], moment_sem),
        ):
            copy = pltpu.make_async_copy(src.at[rows, :], dst.at[there, :], sem.at[tile])
            copy.start()
            copies.append(copy)
    for copy in copies:
        copy.wait()


def on_device(
    normed_inputs, value_cotangent, expert_hidden, expert_cotangent, slot_gate, slot_count,
    expert_weight, expert_moment, value_weight, value_moment,
):
    bf16 = jnp.bfloat16
    in_hbm = pl.BlockSpec(memory_space=pltpu.HBM)
    vmem = pl.BlockSpec(memory_space=pltpu.VMEM)
    dma = pltpu.SemaphoreType.DMA
    grads, moments, weights, factor = pl.pallas_call(
        kernel,
        name="gradients",
        out_shape=(
            pltpu.VMEM((1024, 1024), jnp.float32),
            pltpu.VMEM((1024, 1024), jnp.float32),
            pltpu.VMEM((1024, 1024), bf16),
            pltpu.VMEM((8, 128), jnp.float32),
        ),
        in_specs=[in_hbm] * 10,
        out_specs=(vmem,) * 4,
        scratch_shapes=[
            pltpu.SMEM((4,), jnp.int32),
            pltpu.VMEM((4, 32), bf16),
            pltpu.VMEM((4, 4, 32, 1024), bf16),
            pltpu.VMEM((4, 4, 4, 2, 32, 1024), bf16),
            pltpu.VMEM((2, 4, 32, 1024), bf16),
            pltpu.VMEM((4, 4, 4, 2, 32, 896), bf16),
            pltpu.VMEM((2, 384, 2048), bf16),
            pltpu.VMEM((2, 384, 1024), bf16),
            pltpu.VMEM((4, 4, 128, 1024), bf16),
            pltpu.VMEM((2, 4, 128, 1024), bf16),
            pltpu.VMEM((4, 128, 1024), bf16),
            pltpu.VMEM((128, 1024), bf16),
            pltpu.VMEM((2, 128, 1024), bf16),
            pltpu.VMEM((128, 1024), bf16),
            pltpu.VMEM((25, 8, 128), jnp.float32),
            dma((16,)),
            dma((2,)), dma((2,)),
            dma((9,)), dma((9,)),
            dma((2, 8)), dma((2, 8)),
            dma((8,)), dma((8,)),
            dma((3, 4)), dma((3, 4)),
            dma((15,)), dma((15,)),
            dma((24,)), dma((24,)),
        ],
        compiler_params=pltpu.CompilerParams(
            collective_id=0, has_side_effects=True, vmem_limit_bytes=46 * 1024 * 1024
        ),
        cost_estimate=pl.CostEstimate(
            flops=2 * 896 * 1024 * 4096 + 2 * 2048 * 1024 * 768,
            bytes_accessed=10_000_000,
            transcendentals=0,
        ),
    )(
        pltpu.with_memory_space_constraint(slot_count[0, 0], pltpu.HBM),
        pltpu.with_memory_space_constraint(slot_gate[0, 0], pltpu.HBM),
        pltpu.with_memory_space_constraint(normed_inputs[0, 0].reshape(384, D), pltpu.HBM),
        pltpu.with_memory_space_constraint(value_cotangent[0, 0].reshape(384, KV), pltpu.HBM),
        pltpu.with_memory_space_constraint(expert_hidden[0, 0].reshape(4, 8, 32, 896), pltpu.HBM),
        pltpu.with_memory_space_constraint(expert_cotangent[0, 0], pltpu.HBM),
        pltpu.with_memory_space_constraint(expert_moment[0], pltpu.HBM),
        pltpu.with_memory_space_constraint(expert_weight[0], pltpu.HBM),
        pltpu.with_memory_space_constraint(value_moment[0], pltpu.HBM),
        pltpu.with_memory_space_constraint(value_weight[0], pltpu.HBM),
    )
    expert_weight_next, expert_next, value_weight_next, value_next = pl.pallas_call(
        update_kernel,
        name="update",
        out_shape=(
            jax.ShapeDtypeStruct((896, 1024), bf16),
            jax.ShapeDtypeStruct((896, 1024), jnp.float32),
            jax.ShapeDtypeStruct((128, 1024), bf16),
            jax.ShapeDtypeStruct((128, 1024), jnp.float32),
        ),
        in_specs=[vmem] * 4,
        out_specs=(in_hbm,) * 4,
        scratch_shapes=[
            pltpu.VMEM((1024, 1024), bf16),
            pltpu.VMEM((1024, 1024), jnp.float32),
            dma((8,)),
            dma((8,)),
        ],
        compiler_params=pltpu.CompilerParams(vmem_limit_bytes=24 * 1024 * 1024),
        cost_estimate=pl.CostEstimate(flops=6 * 1024 * 1024, bytes_accessed=6_000_000, transcendentals=0),
    )(
        factor, grads, moments, weights,
    )
    return (expert_weight_next[None], expert_next[None], value_weight_next[None], value_next[None])


def solution(mesh):
    finer = Mesh(mesh.devices.reshape(mesh.shape["section"], 4, 2, 2, 2), AXES)
    specs = (
        P("section", WIDE, NARROW),
        P("section", WIDE, NARROW),
        P("section", WIDE_NARROW, None),
        P("section", WIDE_NARROW, None),
    )
    in_specs = (
        P("section", NARROW, None, WIDE, None),
        P("section", NARROW, None, WIDE, None),
        P("section", NARROW, None, None, WIDE),
        P("section", NARROW, None, WIDE, None),
        P("section", NARROW, None, WIDE),
        P("section", NARROW, None),
    ) + specs
    return jax.shard_map(
        on_device, mesh=finer, in_specs=in_specs, out_specs=specs, check_vma=False
    )
```

```python
import math

import jax
import jax.numpy as jnp
from jax import lax
from jax.experimental import pallas as pl
from jax.experimental.pallas import tpu as pltpu
from jax.sharding import Mesh
from jax.sharding import PartitionSpec as P

D = 4096
FF = 7168
KV = 1024
SECTIONS = 4
ENTRY_COUNT = SECTIONS * (FF * D + D * KV)
AXES = ("section", "wide_0", "wide_1", "narrow_0", "narrow_1")
WIDE = ("wide_0", "wide_1")
NARROW = ("narrow_0", "narrow_1")
WIDE_NARROW = ("wide_0", "wide_1", "narrow_0", "narrow_1")
MESH = pl.DeviceIdType.MESH

MOMENTUM_DECAY = 0.9
STEP_RATE = 0.01

PIECES = ((0, 0), (1, 0), (2, 0), (2, 1), (3, 0), (3, 1), (0, 1), (1, 1))
BY_Z1 = (0, 2, 4, 6)
BY_Z3 = (1, 3, 5, 7)


def flip(value, mask):
    if mask == 0:
        return value
    if mask == 1:
        return value + 1 - 2 * (value % 2)
    if mask == 2:
        return (value + 2) % 4
    return 3 - value


def kernel(
    counts, gates, inputs, value_cot, hidden, cotangent,
    expert_moment, expert_weight, value_moment, value_weight,
    grads_out, moments_out, weights_out, factor_out,
    count_ref, gate_ref, staged, gathered, relay, weights, tokens, token_cots, parts, halves, quarters, cross, eighths, last,
    norms,
    local_sem, token_send, token_recv, cot_send, cot_recv, z_send, z_recv, zf_send, zf_recv,
    hid_send, hid_recv, val_send, val_recv, norm_send, norm_recv, reach_sem,
):
    section = lax.axis_index("section")
    z = lax.axis_index("wide_0")
    hi = lax.axis_index("wide_1")
    lo = lax.axis_index("narrow_0")
    core = lax.axis_index("narrow_1")
    x = 2 * hi + lo
    side = (hi, 1 - hi)

    def device(dy=0, dz=0, dx=0, dc=0):
        there = flip(x, dx)
        return (flip(section, dy), flip(z, dz), there // 2, there % 2, 1 - core if dc else core)

    def send(src, dst, send_sem, recv_sem, **where):
        return pltpu.make_async_remote_copy(
            src_ref=src, dst_ref=dst, send_sem=send_sem, recv_sem=recv_sem,
            device_id=device(**where), device_id_type=MESH,
        )

    pending = []

    def start(copy):
        copy.start()
        pending.append(copy)
        return copy

    peers = [dict(dx=i // 2, dc=i % 2) for i in range(1, 8)]
    peers += [dict(dz=i % 4, dy=i // 4) for i in range(1, 16)]

    small_loads = [
        pltpu.make_async_copy(counts, count_ref, local_sem.at[10]),
        pltpu.make_async_copy(gates, gate_ref, local_sem.at[11]),
    ]
    for load in small_loads:
        load.start()
    cot_loads = []
    for rel in range(4):
        column = (2 * (1 - lo if rel // 2 else lo) + (1 - core if rel % 2 else core)) * 1024
        source = cotangent.at[:, :, pl.ds(pl.multiple_of(column, 1024), 1024)]
        load = pltpu.make_async_copy(source, staged.at[rel], local_sem.at[rel])
        load.start()
        cot_loads.append(load)
    barrier = pltpu.get_barrier_semaphore()
    near = [dict(dc=1), dict(dz=1), dict(dz=3), dict(dy=1), dict(dy=3)]
    near += [dict(dx=dx, dc=dc) for dx in (1, 3) for dc in (0, 1)]
    for peer in near:
        pl.semaphore_signal(barrier, inc=1, device_id=device(**peer), device_id_type=MESH)

    lanes = lax.broadcasted_iota(jnp.int32, (1, 32), 1) + (2 * z + hi) * 32
    diagonal = lax.broadcasted_iota(jnp.int32, (32, 32), 0) == lax.broadcasted_iota(
        jnp.int32, (32, 32), 1
    )
    columns = []
    for load in small_loads:
        load.wait()
    for micro in range(4):
        gate = gate_ref[micro : micro + 1, :].astype(jnp.float32)
        row = jnp.where(lanes < count_ref[micro], gate, jnp.zeros_like(gate))
        square = jnp.where(diagonal, jnp.broadcast_to(row, (32, 32)), 0.0)
        columns.append(jnp.sum(square, axis=1, keepdims=True))

    def scale(rel):
        cot_loads[rel].wait()
        for micro in range(4):
            scaled = (columns[micro] * staged[rel, micro].astype(jnp.float32)).astype(jnp.bfloat16)
            if rel == 0:
                gathered[0, 0, micro, hi] = scaled
            else:
                staged[rel, micro] = scaled

    def spread(step):
        if step:
            pl.semaphore_wait(reach_sem.at[step - 1], 4)
        if step < 3:
            for peer in near[1:5]:
                pl.semaphore_signal(
                    reach_sem.at[step], inc=1, device_id=device(**peer), device_id_type=MESH
                )

    def piece(slot, index):
        replica, far = PIECES[index]
        return gathered.at[slot, replica, :, side[far]]

    def along_z(index):
        start(send(piece(0, index), piece(1, index), z_send.at[0, index], z_recv.at[0, index], dz=1))
        start(send(piece(0, index), piece(3, index), z_send.at[1, index], z_recv.at[1, index], dz=3))

    def z_arrival(link, index):
        slot = (1, 3)[link]
        return send(piece(0, index), piece(slot, index), z_send.at[link, index], z_recv.at[link, index], dz=slot)

    def forward_z(index):
        if index in BY_Z1:
            z_arrival(1, index).wait_recv()
            start(send(piece(3, index), piece(2, index), zf_send.at[index], zf_recv.at[index], dz=1))
        else:
            z_arrival(0, index).wait_recv()
            start(send(piece(1, index), piece(2, index), zf_send.at[index], zf_recv.at[index], dz=3))

    def into(replica, far):
        return gathered.at[0, replica, :, side[far]]

    mine_0 = into(0, 0)
    cot = {}

    def cot_send_of(name, index, src, dst, **where):
        cot[name] = start(send(src, dst, cot_send.at[index], cot_recv.at[index], **where))

    scale(0)
    pl.semaphore_wait(barrier, len(near))
    scale(2)
    along_z(0)
    scale(1)
    cot_send_of("x1_same", 3, staged.at[2], into(2, 0), dx=1)
    cot_send_of("x3_same", 4, staged.at[2], into(2, 0), dx=3)
    cot_send_of("relay_1", 1, mine_0, relay.at[0], dx=1)
    scale(3)
    cot_send_of("core", 0, staged.at[1], into(1, 0), dc=1)
    cot_send_of("relay_3", 2, staged.at[1], relay.at[1], dx=3)
    cot_send_of("x1_cross", 5, staged.at[3], into(3, 0), dx=1, dc=1)
    cot_send_of("x3_cross", 6, staged.at[3], into(3, 0), dx=3, dc=1)

    load_cots = pltpu.make_async_copy(value_cot, token_cots.at[0], local_sem.at[4])
    load_cots.start()
    others = []
    for dx in range(4):
        for dz in range(4):
            block = 2 * (4 * flip(z, dz) + flip(x, dx))
            place = pl.ds((dx * 4 + dz) * 128, 128)
            for which, owner in ((0, core), (1, 1 - core)):
                source = inputs.at[:, pl.ds(pl.multiple_of((block + owner) * 128, 128), 128)]
                if which == 0:
                    pltpu.make_async_copy(source, tokens.at[0, :, place], local_sem.at[5]).start()
                else:
                    others.append((source, place))
    hid_loads = []
    for dz in range(4):
        rows = pl.ds(2 * flip(z, dz), 2)
        load = pltpu.make_async_copy(hidden.at[:, rows], weights.at[0, dz], local_sem.at[6 + dz])
        load.start()
        hid_loads.append(load)
    state_loads = [
        pltpu.make_async_copy(expert_moment, moments_out.at[0:896], local_sem.at[12]),
        pltpu.make_async_copy(expert_weight, weights_out.at[0:896], local_sem.at[13]),
        pltpu.make_async_copy(value_moment, moments_out.at[896:1024], local_sem.at[14]),
        pltpu.make_async_copy(value_weight, weights_out.at[896:1024], local_sem.at[15]),
    ]

    spread(0)
    for source, place in others:
        send(source, tokens.at[1, :, place], token_send.at[0], token_recv.at[0], dc=1).start()
    token_whole = send(tokens.at[1], tokens.at[1], token_send.at[0], token_recv.at[0], dc=1)
    pending.append(token_whole)
    cots_whole = start(send(value_cot, token_cots.at[1], token_send.at[1], token_recv.at[1], dc=1))
    hid_core = []
    for dz in range(4):
        rows = pl.ds(2 * flip(z, dz), 2)
        hid_core.append(
            start(send(hidden.at[:, rows], weights.at[1, dz], hid_send.at[0, dz], hid_recv.at[0, dz], dc=1))
        )

    cot["core"].wait_recv()
    along_z(1)

    load_cots.wait()
    pltpu.make_async_copy(tokens.at[0], tokens.at[0], local_sem.at[5]).wait()
    token_whole.wait_recv()
    cots_whole.wait_recv()

    def value_parts(dx):
        def block(dz, carry):
            place = pl.ds(pl.multiple_of((dx * 4 + dz) * 128, 128), 128)
            lhs = tokens[:, :, place].reshape(768, 128)
            rhs = token_cots[...].reshape(768, KV)
            product = lax.dot_general(
                lhs, rhs, (((0,), (0,)), ((), ())), preferred_element_type=jnp.float32
            )
            parts[dx, dz] = product.astype(jnp.bfloat16)
            return carry

        lax.fori_loop(0, 4, block, 0)

    value = {}

    def value_send(name, index, src, dst, **where):
        value[name] = start(send(src, dst, val_send.at[index], val_recv.at[index], **where))

    hid_far = {}

    def send_hidden(dz):
        hid_loads[dz].wait()
        hid_far[dz] = start(
            send(weights.at[0, dz], weights.at[2, dz], hid_send.at[1, dz], hid_recv.at[1, dz], dx=1)
        )

    value_parts(2)
    cot["x1_same"].wait_recv()
    along_z(2)
    cot["x3_same"].wait_recv()
    along_z(3)
    value_parts(3)
    cot["relay_1"].wait_recv()
    cot_send_of("far_3", 7, relay.at[0], into(0, 0), dx=3)
    cot["relay_3"].wait_recv()
    cot_send_of("far_1", 8, relay.at[1], into(1, 1), dx=1, dc=1)
    for dz in (0, 1, 3):
        send_hidden(dz)
    for i, (far, dz) in enumerate(((1, 2), (0, 2), (1, 1), (1, 3), (1, 0), (0, 3), (0, 1), (0, 0))):
        value_send(("x3", far, dz), i, parts.at[3 - far, dz], halves.at[far, dz], dx=3)
    for load in state_loads:
        load.start()
    spread(1)
    value_parts(1)
    cot["x1_cross"].wait_recv()
    along_z(4)
    cot["x3_cross"].wait_recv()
    along_z(5)
    value_parts(0)
    spread(2)
    cot["far_3"].wait_recv()
    along_z(6)
    cot["far_1"].wait_recv()
    along_z(7)

    def accumulate(weights_of, gathered_of, first=False):
        def tile(n, carry):
            place = pl.ds(pl.multiple_of(n * 256, 256), 256)
            lhs = weights_of().reshape(256, 896)
            rhs = gathered_of(place).reshape(256, 256)
            product = lax.dot_general(
                lhs, rhs, (((0,), (0,)), ((), ())), preferred_element_type=jnp.float32
            )
            if first:
                grads_out[0:896, place] = product
            else:
                grads_out[0:896, place] += product
            return carry

        lax.fori_loop(0, 4, tile, 0)

    def products(slot, replica, first=False):
        accumulate(
            lambda: weights[replica, slot],
            lambda place: gathered[slot, replica, :, :, :, place],
            first,
        )

    def chip_products(slot, far):
        accumulate(
            lambda: weights[0:2, slot, :, side[far]],
            lambda place: gathered[slot, 0:2, :, side[far], :, place],
        )

    def second_step(dz, more=None):
        value[("x3", 1, dz)].wait_recv()
        total = parts[1, dz].astype(jnp.float32) + halves[1, dz].astype(jnp.float32)
        if more is not None:
            total = total + more[...].astype(jnp.float32)
        parts[1, dz] = total.astype(jnp.bfloat16)

    def second_send(dz):
        value_send(("x1", dz), 8 + dz, parts.at[1, dz], quarters.at[dz], dx=1)

    hid_pass = {}

    def pass_hidden(dz):
        hid_far[dz].wait_recv()
        hid_pass[dz] = start(
            send(weights.at[2, dz], weights.at[3, dz], hid_send.at[2, dz], hid_recv.at[2, dz], dc=1)
        )

    def far_arrival(index):
        if index in BY_Z1:
            send(piece(3, index), piece(2, index), zf_send.at[index], zf_recv.at[index], dz=1).wait_recv()
        else:
            send(piece(1, index), piece(2, index), zf_send.at[index], zf_recv.at[index], dz=3).wait_recv()

    def third_step(dz):
        value[("x3", 0, dz)].wait_recv()
        total = parts[0, dz].astype(jnp.float32) + halves[0, dz].astype(jnp.float32)
        if dz != 2:
            value[("x1", dz)].wait_recv()
            total = total + quarters[dz].astype(jnp.float32)
        return total

    products(0, 0, first=True)
    second_step(2)
    hid_core[0].wait_recv()
    products(0, 1)
    value_send("cross", 10, parts.at[1, 2], cross, dz=3)
    parts[0, 2] = third_step(2).astype(jnp.bfloat16)
    forward_z(0)
    forward_z(1)
    value_send("z1_1", 13, parts.at[0, 2], eighths.at[1], dz=1)
    forward_z(2)
    forward_z(3)
    forward_z(4)
    pass_hidden(0)
    products(0, 2)
    forward_z(5)
    hid_pass[0].wait_recv()
    products(0, 3)
    forward_z(6)
    pass_hidden(1)
    second_step(3)
    forward_z(7)
    second_send(3)
    z_arrival(0, 0).wait_recv()
    z_arrival(0, 6).wait_recv()
    products(1, 0)
    second_step(0)
    value["cross"].wait_recv()
    second_step(1, cross)
    hid_core[1].wait_recv()
    z_arrival(1, 1).wait_recv()
    z_arrival(1, 7).wait_recv()
    products(1, 1)
    second_send(1)
    send_hidden(2)
    second_send(0)
    z_arrival(0, 2).wait_recv()
    products(1, 2)
    pass_hidden(3)
    hid_pass[1].wait_recv()
    z_arrival(0, 4).wait_recv()
    products(1, 3)
    third = third_step(3)
    value["z1_1"].wait_recv()
    parts[0, 3] = (third + eighths[1].astype(jnp.float32)).astype(jnp.bfloat16)
    products(3, 0)
    value_send("z3", 14, parts.at[0, 3], last, dz=3)
    parts[0, 1] = third_step(1).astype(jnp.bfloat16)
    hid_core[3].wait_recv()
    products(3, 1)
    value_send("z1_0", 12, parts.at[0, 1], eighths.at[0], dz=1)
    z_arrival(1, 3).wait_recv()
    products(3, 2)
    hid_pass[3].wait_recv()
    z_arrival(1, 5).wait_recv()
    products(3, 3)
    hid_core[2].wait_recv()
    far_arrival(0)
    far_arrival(1)
    chip_products(2, 0)
    pass_hidden(2)
    far_arrival(2)
    far_arrival(3)
    products(2, 2)
    hid_pass[2].wait_recv()
    far_arrival(4)
    far_arrival(5)
    products(2, 3)
    far_arrival(6)
    far_arrival(7)
    chip_products(2, 1)

    def squares(first, rows):
        def tile(i, totals):
            chunk = grads_out[pl.ds(pl.multiple_of(first + i * 32, 32), 32), :]
            totals = list(totals)
            for group in range(4):
                for n in range(8):
                    one = chunk[group * 8 : (group + 1) * 8, n * 128 : (n + 1) * 128]
                    totals[n] = totals[n] + one * one
            return tuple(totals)

        totals = lax.fori_loop(0, rows // 32, tile, (jnp.zeros((8, 128), jnp.float32),) * 8)
        return sum(totals[1:], totals[0])

    spread(3)
    expert_squares = squares(0, 896)
    for load in state_loads:
        load.wait()
    near = third_step(0)
    value["z1_0"].wait_recv()
    near = near + eighths[0].astype(jnp.float32)
    value["z3"].wait_recv()
    grads_out[896:1024, :] = near + last[...].astype(jnp.float32)
    norms[0] = expert_squares + squares(896, 128)
    started = len(pending)

    base = 0
    slot = 1
    for group in (peers[:7], peers[7:]):
        copies = []
        for i, peer in enumerate(group):
            copies.append(
                start(
                    send(norms.at[base], norms.at[slot + i], norm_send.at[slot + i], norm_recv.at[slot + i], **peer)
                )
            )
        if base == 0:
            for copy in pending[:started]:
                copy.wait_send()
        total = norms[base]
        for i, copy in enumerate(copies):
            copy.wait_recv()
            total = total + norms[slot + i]
        base = slot + len(group)
        norms[base] = total
        slot = base + 1
    overall = jnp.sum(jnp.sum(norms[base], axis=0, keepdims=True), axis=1, keepdims=True)
    overall = jnp.broadcast_to(overall, (8, 128))
    factor_out[...] = jnp.minimum(1.0, math.sqrt(ENTRY_COUNT) / jnp.sqrt(overall + 1e-06))

    for copy in pending[started:]:
        copy.wait_send()


def update_kernel(
    factor_ref, grads, moments, weights,
    expert_weight_out, expert_moment_out, value_weight_out, value_moment_out,
    new_weights, new_moments, weight_sem, moment_sem,
):
    factor = factor_ref[0:1, 0:1]
    copies = []
    for tile in range(8):

        def chunk(i, carry, tile=tile):
            at = pl.ds(pl.multiple_of(tile * 128 + i * 32, 32), 32)
            moved = MOMENTUM_DECAY * moments[at, :] + factor * grads[at, :]
            new_moments[at, :] = moved
            new_weights[at, :] = (weights[at, :].astype(jnp.float32) - STEP_RATE * moved).astype(
                jnp.bfloat16
            )
            return carry

        lax.fori_loop(0, 4, chunk, 0)
        rows = pl.ds(tile * 128, 128)
        there = rows if tile < 7 else pl.ds(0, 128)
        outs = (expert_weight_out, expert_moment_out) if tile < 7 else (value_weight_out, value_moment_out)
        for src, dst, sem in (
            (new_weights, outs[0], weight_sem),
            (new_moments, outs[1], moment_sem),
        ):
            copy = pltpu.make_async_copy(src.at[rows, :], dst.at[there, :], sem.at[tile])
            copy.start()
            copies.append(copy)
    for copy in copies:
        copy.wait()


def on_device(
    normed_inputs, value_cotangent, expert_hidden, expert_cotangent, slot_gate, slot_count,
    expert_weight, expert_moment, value_weight, value_moment,
):
    bf16 = jnp.bfloat16
    in_hbm = pl.BlockSpec(memory_space=pltpu.HBM)
    vmem = pl.BlockSpec(memory_space=pltpu.VMEM)
    dma = pltpu.SemaphoreType.DMA
    grads, moments, weights, factor = pl.pallas_call(
        kernel,
        name="gradients",
        out_shape=(
            pltpu.VMEM((1024, 1024), jnp.float32),
            pltpu.VMEM((1024, 1024), jnp.float32),
            pltpu.VMEM((1024, 1024), bf16),
            pltpu.VMEM((8, 128), jnp.float32),
        ),
        in_specs=[in_hbm] * 10,
        out_specs=(vmem,) * 4,
        scratch_shapes=[
            pltpu.SMEM((4,), jnp.int32),
            pltpu.VMEM((4, 32), bf16),
            pltpu.VMEM((4, 4, 32, 1024), bf16),
            pltpu.VMEM((4, 4, 4, 2, 32, 1024), bf16),
            pltpu.VMEM((2, 4, 32, 1024), bf16),
            pltpu.VMEM((4, 4, 4, 2, 32, 896), bf16),
            pltpu.VMEM((2, 384, 2048), bf16),
            pltpu.VMEM((2, 384, 1024), bf16),
            pltpu.VMEM((4, 4, 128, 1024), bf16),
            pltpu.VMEM((2, 4, 128, 1024), bf16),
            pltpu.VMEM((4, 128, 1024), bf16),
            pltpu.VMEM((128, 1024), bf16),
            pltpu.VMEM((2, 128, 1024), bf16),
            pltpu.VMEM((128, 1024), bf16),
            pltpu.VMEM((25, 8, 128), jnp.float32),
            dma((16,)),
            dma((2,)), dma((2,)),
            dma((9,)), dma((9,)),
            dma((2, 8)), dma((2, 8)),
            dma((8,)), dma((8,)),
            dma((3, 4)), dma((3, 4)),
            dma((15,)), dma((15,)),
            dma((24,)), dma((24,)),
            pltpu.SemaphoreType.REGULAR((3,)),
        ],
        compiler_params=pltpu.CompilerParams(
            collective_id=0, has_side_effects=True, vmem_limit_bytes=46 * 1024 * 1024
        ),
        cost_estimate=pl.CostEstimate(
            flops=2 * 896 * 1024 * 4096 + 2 * 2048 * 1024 * 768,
            bytes_accessed=10_000_000,
            transcendentals=0,
        ),
    )(
        pltpu.with_memory_space_constraint(slot_count[0, 0], pltpu.HBM),
        pltpu.with_memory_space_constraint(slot_gate[0, 0], pltpu.HBM),
        pltpu.with_memory_space_constraint(normed_inputs[0, 0].reshape(384, D), pltpu.HBM),
        pltpu.with_memory_space_constraint(value_cotangent[0, 0].reshape(384, KV), pltpu.HBM),
        pltpu.with_memory_space_constraint(expert_hidden[0, 0].reshape(4, 8, 32, 896), pltpu.HBM),
        pltpu.with_memory_space_constraint(expert_cotangent[0, 0], pltpu.HBM),
        pltpu.with_memory_space_constraint(expert_moment[0], pltpu.HBM),
        pltpu.with_memory_space_constraint(expert_weight[0], pltpu.HBM),
        pltpu.with_memory_space_constraint(value_moment[0], pltpu.HBM),
        pltpu.with_memory_space_constraint(value_weight[0], pltpu.HBM),
    )
    expert_weight_next, expert_next, value_weight_next, value_next = pl.pallas_call(
        update_kernel,
        name="update",
        out_shape=(
            jax.ShapeDtypeStruct((896, 1024), bf16),
            jax.ShapeDtypeStruct((896, 1024), jnp.float32),
            jax.ShapeDtypeStruct((128, 1024), bf16),
            jax.ShapeDtypeStruct((128, 1024), jnp.float32),
        ),
        in_specs=[vmem] * 4,
        out_specs=(in_hbm,) * 4,
        scratch_shapes=[
            pltpu.VMEM((1024, 1024), bf16),
            pltpu.VMEM((1024, 1024), jnp.float32),
            dma((8,)),
            dma((8,)),
        ],
        compiler_params=pltpu.CompilerParams(vmem_limit_bytes=24 * 1024 * 1024),
        cost_estimate=pl.CostEstimate(flops=6 * 1024 * 1024, bytes_accessed=6_000_000, transcendentals=0),
    )(
        factor, grads, moments, weights,
    )
    return (expert_weight_next[None], expert_next[None], value_weight_next[None], value_next[None])


def solution(mesh):
    finer = Mesh(mesh.devices.reshape(mesh.shape["section"], 4, 2, 2, 2), AXES)
    specs = (
        P("section", WIDE, NARROW),
        P("section", WIDE, NARROW),
        P("section", WIDE_NARROW, None),
        P("section", WIDE_NARROW, None),
    )
    in_specs = (
        P("section", NARROW, None, WIDE, None),
        P("section", NARROW, None, WIDE, None),
        P("section", NARROW, None, None, WIDE),
        P("section", NARROW, None, WIDE, None),
        P("section", NARROW, None, WIDE),
        P("section", NARROW, None),
    ) + specs
    return jax.shard_map(
        on_device, mesh=finer, in_specs=in_specs, out_specs=specs, check_vma=False
    )
```

```python
import math

import jax
import jax.numpy as jnp
from jax import lax
from jax.experimental import pallas as pl
from jax.experimental.pallas import tpu as pltpu
from jax.sharding import Mesh
from jax.sharding import PartitionSpec as P

D = 4096
FF = 7168
KV = 1024
SECTIONS = 4
ENTRY_COUNT = SECTIONS * (FF * D + D * KV)
AXES = ("section", "wide_0", "wide_1", "narrow_0", "narrow_1")
WIDE = ("wide_0", "wide_1")
NARROW = ("narrow_0", "narrow_1")
WIDE_NARROW = ("wide_0", "wide_1", "narrow_0", "narrow_1")
MESH = pl.DeviceIdType.MESH

TILE = 128

MOMENTUM_DECAY = 0.9
STEP_RATE = 0.01

PIECES = ((0, 0), (1, 0), (2, 0), (2, 1), (3, 0), (3, 1), (0, 1), (1, 1))
BY_Z1 = (0, 2, 4, 6)
BY_Z3 = (1, 3, 5, 7)


def flip(value, mask):
    if mask == 0:
        return value
    if mask == 1:
        return value + 1 - 2 * (value % 2)
    if mask == 2:
        return (value + 2) % 4
    return 3 - value


def kernel(
    counts, gates, inputs, value_cot, hidden, cotangent,
    expert_moment, expert_weight, value_moment, value_weight,
    grads_out, moments_out, weights_out, factor_out,
    count_ref, gate_ref, staged, gathered, relay, weights, tokens, token_cots, parts, halves, quarters, cross, eighths, last,
    norms,
    local_sem, token_send, token_recv, cot_send, cot_recv, z_send, z_recv, zf_send, zf_recv,
    hid_send, hid_recv, val_send, val_recv, norm_send, norm_recv, reach_sem,
):
    section = lax.axis_index("section")
    z = lax.axis_index("wide_0")
    hi = lax.axis_index("wide_1")
    lo = lax.axis_index("narrow_0")
    core = lax.axis_index("narrow_1")
    x = 2 * hi + lo
    side = (hi, 1 - hi)

    def device(dy=0, dz=0, dx=0, dc=0):
        there = flip(x, dx)
        return (flip(section, dy), flip(z, dz), there // 2, there % 2, 1 - core if dc else core)

    def send(src, dst, send_sem, recv_sem, **where):
        return pltpu.make_async_remote_copy(
            src_ref=src, dst_ref=dst, send_sem=send_sem, recv_sem=recv_sem,
            device_id=device(**where), device_id_type=MESH,
        )

    pending = []

    def start(copy):
        copy.start()
        pending.append(copy)
        return copy

    row_peers = [dict(dx=dx, dc=dc) for dx, dc in ((2, 1), (2, 0), (1, 1), (3, 1), (1, 0), (3, 0), (0, 1))]
    far_peers = [dict(dz=i % 4, dy=i // 4) for i in (10, 6, 14, 9, 11, 2, 8, 5, 7, 13, 15, 1, 3, 4, 12)]

    small_loads = [
        pltpu.make_async_copy(counts, count_ref, local_sem.at[10]),
        pltpu.make_async_copy(gates, gate_ref, local_sem.at[11]),
    ]
    for load in small_loads:
        load.start()
    cot_loads = []
    for rel in range(4):
        column = (2 * (1 - lo if rel // 2 else lo) + (1 - core if rel % 2 else core)) * 1024
        source = cotangent.at[:, :, pl.ds(pl.multiple_of(column, 1024), 1024)]
        load = pltpu.make_async_copy(source, staged.at[rel], local_sem.at[rel])
        load.start()
        cot_loads.append(load)
    barrier = pltpu.get_barrier_semaphore()
    near = [dict(dc=1), dict(dz=1), dict(dz=3), dict(dy=1), dict(dy=3)]
    near += [dict(dx=dx, dc=dc) for dx in (1, 3) for dc in (0, 1)]
    for peer in near:
        pl.semaphore_signal(barrier, inc=1, device_id=device(**peer), device_id_type=MESH)

    lanes = lax.broadcasted_iota(jnp.int32, (1, 32), 1) + (2 * z + hi) * 32
    diagonal = lax.broadcasted_iota(jnp.int32, (32, 32), 0) == lax.broadcasted_iota(
        jnp.int32, (32, 32), 1
    )
    columns = []
    for load in small_loads:
        load.wait()
    for micro in range(4):
        gate = gate_ref[micro : micro + 1, :].astype(jnp.float32)
        row = jnp.where(lanes < count_ref[micro], gate, jnp.zeros_like(gate))
        square = jnp.where(diagonal, jnp.broadcast_to(row, (32, 32)), 0.0)
        columns.append(jnp.sum(square, axis=1, keepdims=True))

    def scale(rel):
        cot_loads[rel].wait()
        for micro in range(4):
            scaled = (columns[micro] * staged[rel, micro].astype(jnp.float32)).astype(jnp.bfloat16)
            if rel == 0:
                gathered[0, 0, micro, hi] = scaled
            else:
                staged[rel, micro] = scaled

    def spread(step):
        if step:
            pl.semaphore_wait(reach_sem.at[step - 1], 4)
        if step < 3:
            for peer in near[1:5]:
                pl.semaphore_signal(
                    reach_sem.at[step], inc=1, device_id=device(**peer), device_id_type=MESH
                )

    def piece(slot, index):
        replica, far = PIECES[index]
        return gathered.at[slot, replica, :, side[far]]

    def along_z(index):
        start(send(piece(0, index), piece(1, index), z_send.at[0, index], z_recv.at[0, index], dz=1))
        start(send(piece(0, index), piece(3, index), z_send.at[1, index], z_recv.at[1, index], dz=3))

    def z_arrival(link, index):
        slot = (1, 3)[link]
        return send(piece(0, index), piece(slot, index), z_send.at[link, index], z_recv.at[link, index], dz=slot)

    def forward_z(index):
        if index in BY_Z1:
            z_arrival(1, index).wait_recv()
            start(send(piece(3, index), piece(2, index), zf_send.at[index], zf_recv.at[index], dz=1))
        else:
            z_arrival(0, index).wait_recv()
            start(send(piece(1, index), piece(2, index), zf_send.at[index], zf_recv.at[index], dz=3))

    def into(replica, far):
        return gathered.at[0, replica, :, side[far]]

    mine_0 = into(0, 0)
    cot = {}

    def cot_send_of(name, index, src, dst, **where):
        cot[name] = start(send(src, dst, cot_send.at[index], cot_recv.at[index], **where))

    scale(0)
    pl.semaphore_wait(barrier, len(near))
    scale(2)
    along_z(0)
    cot_send_of("x1_same", 3, staged.at[2], into(2, 0), dx=1)
    cot_send_of("x3_same", 4, staged.at[2], into(2, 0), dx=3)
    cot_send_of("relay_1", 1, mine_0, relay.at[0], dx=1)
    scale(1)
    scale(3)
    cot_send_of("core", 0, staged.at[1], into(1, 0), dc=1)
    cot_send_of("relay_3", 2, staged.at[1], relay.at[1], dx=3)
    cot_send_of("x1_cross", 5, staged.at[3], into(3, 0), dx=1, dc=1)
    cot_send_of("x3_cross", 6, staged.at[3], into(3, 0), dx=3, dc=1)

    load_cots = pltpu.make_async_copy(value_cot, token_cots.at[0], local_sem.at[4])
    load_cots.start()
    others = []
    for dx in range(4):
        for dz in range(4):
            block = 2 * (4 * flip(z, dz) + flip(x, dx))
            place = pl.ds((dx * 4 + dz) * 128, 128)
            for which, owner in ((0, core), (1, 1 - core)):
                source = inputs.at[:, pl.ds(pl.multiple_of((block + owner) * 128, 128), 128)]
                if which == 0:
                    pltpu.make_async_copy(source, tokens.at[0, :, place], local_sem.at[5]).start()
                else:
                    others.append((source, place))
    hid_loads = []
    for dz in range(4):
        rows = pl.ds(2 * flip(z, dz), 2)
        load = pltpu.make_async_copy(hidden.at[:, rows], weights.at[0, dz], local_sem.at[6 + dz])
        load.start()
        hid_loads.append(load)
    state_loads = [
        pltpu.make_async_copy(expert_moment, moments_out.at[0:896], local_sem.at[12]),
        pltpu.make_async_copy(expert_weight, weights_out.at[0:896], local_sem.at[13]),
        pltpu.make_async_copy(value_moment, moments_out.at[896:1024], local_sem.at[14]),
        pltpu.make_async_copy(value_weight, weights_out.at[896:1024], local_sem.at[15]),
    ]

    spread(0)
    for source, place in others:
        send(source, tokens.at[1, :, place], token_send.at[0], token_recv.at[0], dc=1).start()
    token_whole = send(tokens.at[1], tokens.at[1], token_send.at[0], token_recv.at[0], dc=1)
    pending.append(token_whole)
    cots_whole = start(send(value_cot, token_cots.at[1], token_send.at[1], token_recv.at[1], dc=1))
    hid_core = []
    for dz in range(4):
        rows = pl.ds(2 * flip(z, dz), 2)
        hid_core.append(
            start(send(hidden.at[:, rows], weights.at[1, dz], hid_send.at[0, dz], hid_recv.at[0, dz], dc=1))
        )

    cot["core"].wait_recv()
    along_z(1)

    load_cots.wait()
    pltpu.make_async_copy(tokens.at[0], tokens.at[0], local_sem.at[5]).wait()
    token_whole.wait_recv()
    cots_whole.wait_recv()

    def value_parts(dx):
        def block(dz, carry):
            place = pl.ds(pl.multiple_of((dx * 4 + dz) * 128, 128), 128)
            lhs = tokens[:, :, place].reshape(768, 128)
            rhs = token_cots[...].reshape(768, KV)
            product = lax.dot_general(
                lhs, rhs, (((0,), (0,)), ((), ())), preferred_element_type=jnp.float32
            )
            parts[dx, dz] = product.astype(jnp.bfloat16)
            return carry

        lax.fori_loop(0, 4, block, 0)

    value = {}

    def value_send(name, index, src, dst, **where):
        value[name] = start(send(src, dst, val_send.at[index], val_recv.at[index], **where))

    hid_far = {}

    def send_hidden(dz):
        hid_loads[dz].wait()
        hid_far[dz] = start(
            send(weights.at[0, dz], weights.at[2, dz], hid_send.at[1, dz], hid_recv.at[1, dz], dx=1)
        )

    value_parts(2)
    cot["x1_same"].wait_recv()
    along_z(2)
    cot["x3_same"].wait_recv()
    along_z(3)
    value_parts(3)
    cot["relay_1"].wait_recv()
    cot_send_of("far_3", 7, relay.at[0], into(0, 0), dx=3)
    cot["relay_3"].wait_recv()
    cot_send_of("far_1", 8, relay.at[1], into(1, 1), dx=1, dc=1)
    for dz in (0, 1, 3):
        send_hidden(dz)
    for i, (far, dz) in enumerate(((1, 2), (0, 2), (1, 1), (1, 3), (1, 0), (0, 3), (0, 1), (0, 0))):
        value_send(("x3", far, dz), i, parts.at[3 - far, dz], halves.at[far, dz], dx=3)
    for load in state_loads:
        load.start()
    spread(1)
    value_parts(1)
    cot["x1_cross"].wait_recv()
    along_z(4)
    cot["x3_cross"].wait_recv()
    along_z(5)
    value_parts(0)
    spread(2)
    cot["far_3"].wait_recv()
    along_z(6)
    cot["far_1"].wait_recv()
    along_z(7)

    def accumulate(weights_of, gathered_of, first=False):
        def tile(n, carry):
            place = pl.ds(pl.multiple_of(n * 256, 256), 256)
            lhs = weights_of().reshape(256, 896)
            rhs = gathered_of(place).reshape(256, 256)
            product = lax.dot_general(
                lhs, rhs, (((0,), (0,)), ((), ())), preferred_element_type=jnp.float32
            )
            if first:
                grads_out[0:896, place] = product
            else:
                grads_out[0:896, place] += product
            return carry

        lax.fori_loop(0, 4, tile, 0)

    def products(slot, replica, first=False):
        accumulate(
            lambda: weights[replica, slot],
            lambda place: gathered[slot, replica, :, :, :, place],
            first,
        )

    def chip_products(slot, far):
        accumulate(
            lambda: weights[0:2, slot, :, side[far]],
            lambda place: gathered[slot, 0:2, :, side[far], :, place],
        )

    def second_step(dz, more=None):
        value[("x3", 1, dz)].wait_recv()
        total = parts[1, dz].astype(jnp.float32) + halves[1, dz].astype(jnp.float32)
        if more is not None:
            total = total + more[...].astype(jnp.float32)
        parts[1, dz] = total.astype(jnp.bfloat16)

    def second_send(dz):
        value_send(("x1", dz), 8 + dz, parts.at[1, dz], quarters.at[dz], dx=1)

    hid_pass = {}

    def pass_hidden(dz):
        hid_far[dz].wait_recv()
        hid_pass[dz] = start(
            send(weights.at[2, dz], weights.at[3, dz], hid_send.at[2, dz], hid_recv.at[2, dz], dc=1)
        )

    def far_arrival(index):
        if index in BY_Z1:
            send(piece(3, index), piece(2, index), zf_send.at[index], zf_recv.at[index], dz=1).wait_recv()
        else:
            send(piece(1, index), piece(2, index), zf_send.at[index], zf_recv.at[index], dz=3).wait_recv()

    def third_step(dz):
        value[("x3", 0, dz)].wait_recv()
        total = parts[0, dz].astype(jnp.float32) + halves[0, dz].astype(jnp.float32)
        if dz != 2:
            value[("x1", dz)].wait_recv()
            total = total + quarters[dz].astype(jnp.float32)
        return total

    products(0, 0, first=True)
    second_step(2)
    hid_core[0].wait_recv()
    products(0, 1)
    value_send("cross", 10, parts.at[1, 2], cross, dz=3)
    parts[0, 2] = third_step(2).astype(jnp.bfloat16)
    forward_z(0)
    forward_z(1)
    value_send("z1_1", 13, parts.at[0, 2], eighths.at[1], dz=1)
    forward_z(2)
    forward_z(3)
    forward_z(4)
    pass_hidden(0)
    products(0, 2)
    forward_z(5)
    hid_pass[0].wait_recv()
    products(0, 3)
    forward_z(6)
    pass_hidden(1)
    second_step(3)
    forward_z(7)
    drained = len(pending)
    second_send(3)
    z_arrival(0, 0).wait_recv()
    z_arrival(0, 6).wait_recv()
    products(1, 0)
    second_step(0)
    value["cross"].wait_recv()
    second_step(1, cross)
    hid_core[1].wait_recv()
    z_arrival(1, 1).wait_recv()
    z_arrival(1, 7).wait_recv()
    products(1, 1)
    second_send(1)
    send_hidden(2)
    second_send(0)
    z_arrival(0, 2).wait_recv()
    products(1, 2)
    pass_hidden(3)
    hid_pass[1].wait_recv()
    z_arrival(0, 4).wait_recv()
    products(1, 3)
    third = third_step(3)
    value["z1_1"].wait_recv()
    parts[0, 3] = (third + eighths[1].astype(jnp.float32)).astype(jnp.bfloat16)
    products(3, 0)
    value_send("z3", 14, parts.at[0, 3], last, dz=3)
    parts[0, 1] = third_step(1).astype(jnp.bfloat16)
    hid_core[3].wait_recv()
    products(3, 1)
    value_send("z1_0", 12, parts.at[0, 1], eighths.at[0], dz=1)
    z_arrival(1, 3).wait_recv()
    products(3, 2)
    hid_pass[3].wait_recv()
    z_arrival(1, 5).wait_recv()
    products(3, 3)
    hid_core[2].wait_recv()
    far_arrival(0)
    far_arrival(1)
    chip_products(2, 0)
    pass_hidden(2)
    far_arrival(2)
    far_arrival(3)
    products(2, 2)
    hid_pass[2].wait_recv()
    far_arrival(4)
    far_arrival(5)
    products(2, 3)
    for copy in pending[:drained]:
        copy.wait_send()
    far_arrival(6)
    far_arrival(7)
    chip_products(2, 1)

    def squares(first, rows):
        def tile(i, totals):
            chunk = grads_out[pl.ds(pl.multiple_of(first + i * 32, 32), 32), :]
            totals = list(totals)
            for group in range(4):
                for n in range(8):
                    one = chunk[group * 8 : (group + 1) * 8, n * 128 : (n + 1) * 128]
                    totals[n] = totals[n] + one * one
            return tuple(totals)

        totals = lax.fori_loop(0, rows // 32, tile, (jnp.zeros((8, 128), jnp.float32),) * 8)
        return sum(totals[1:], totals[0])

    spread(3)
    expert_squares = squares(0, 896)
    for load in state_loads:
        load.wait()
    near = third_step(0)
    value["z1_0"].wait_recv()
    near = near + eighths[0].astype(jnp.float32)
    value["z3"].wait_recv()
    grads_out[896:1024, :] = near + last[...].astype(jnp.float32)
    norms[0] = jnp.sum(expert_squares + squares(896, 128), axis=0, keepdims=True)
    started = len(pending)

    base = 0
    slot = 1
    for group in (row_peers, far_peers):
        copies = []
        for i, peer in enumerate(group):
            copies.append(
                start(
                    send(norms.at[base], norms.at[slot + i], norm_send.at[slot + i], norm_recv.at[slot + i], **peer)
                )
            )
        if base == 0:
            for copy in pending[drained:started]:
                copy.wait_send()
        total = norms[base]
        for i, copy in reversed(tuple(enumerate(copies))):
            copy.wait_recv()
            total = total + norms[slot + i]
        base = slot + len(group)
        norms[base] = total
        slot = base + 1
    overall = jnp.sum(norms[base], axis=1, keepdims=True)
    overall = jnp.broadcast_to(overall, (8, 128))
    factor_out[...] = jnp.minimum(1.0, math.sqrt(ENTRY_COUNT) / jnp.sqrt(overall + 1e-06))

    for copy in pending[started:]:
        copy.wait_send()


def update_kernel(
    factor_ref, grads, moments, weights,
    expert_weight_out, expert_moment_out, value_weight_out, value_moment_out,
    new_weights, new_moments, weight_sem, moment_sem,
):
    factor = factor_ref[0:1, 0:1]
    copies = []
    for tile in range(1024 // TILE):

        def chunk(i, carry, tile=tile):
            at = pl.ds(pl.multiple_of(tile * TILE + i * 32, 32), 32)
            moved = MOMENTUM_DECAY * moments[at, :] + factor * grads[at, :]
            new_moments[at, :] = moved
            new_weights[at, :] = (weights[at, :].astype(jnp.float32) - STEP_RATE * moved).astype(
                jnp.bfloat16
            )
            return carry

        lax.fori_loop(0, TILE // 32, chunk, 0)
        rows = pl.ds(tile * TILE, TILE)
        expert = tile * TILE < 896
        there = rows if expert else pl.ds(tile * TILE - 896, TILE)
        outs = (expert_weight_out, expert_moment_out) if expert else (value_weight_out, value_moment_out)
        for src, dst, sem in (
            (new_weights, outs[0], weight_sem),
            (new_moments, outs[1], moment_sem),
        ):
            copy = pltpu.make_async_copy(src.at[rows, :], dst.at[there, :], sem.at[tile])
            copy.start()
            copies.append(copy)
    for copy in copies:
        copy.wait()


def on_device(
    normed_inputs, value_cotangent, expert_hidden, expert_cotangent, slot_gate, slot_count,
    expert_weight, expert_moment, value_weight, value_moment,
):
    bf16 = jnp.bfloat16
    in_hbm = pl.BlockSpec(memory_space=pltpu.HBM)
    vmem = pl.BlockSpec(memory_space=pltpu.VMEM)
    dma = pltpu.SemaphoreType.DMA
    grads, moments, weights, factor = pl.pallas_call(
        kernel,
        name="gradients",
        out_shape=(
            pltpu.VMEM((1024, 1024), jnp.float32),
            pltpu.VMEM((1024, 1024), jnp.float32),
            pltpu.VMEM((1024, 1024), bf16),
            pltpu.VMEM((8, 128), jnp.float32),
        ),
        in_specs=[in_hbm] * 10,
        out_specs=(vmem,) * 4,
        scratch_shapes=[
            pltpu.SMEM((4,), jnp.int32),
            pltpu.VMEM((4, 32), bf16),
            pltpu.VMEM((4, 4, 32, 1024), bf16),
            pltpu.VMEM((4, 4, 4, 2, 32, 1024), bf16),
            pltpu.VMEM((2, 4, 32, 1024), bf16),
            pltpu.VMEM((4, 4, 4, 2, 32, 896), bf16),
            pltpu.VMEM((2, 384, 2048), bf16),
            pltpu.VMEM((2, 384, 1024), bf16),
            pltpu.VMEM((4, 4, 128, 1024), bf16),
            pltpu.VMEM((2, 4, 128, 1024), bf16),
            pltpu.VMEM((4, 128, 1024), bf16),
            pltpu.VMEM((128, 1024), bf16),
            pltpu.VMEM((2, 128, 1024), bf16),
            pltpu.VMEM((128, 1024), bf16),
            pltpu.VMEM((25, 1, 128), jnp.float32),
            dma((16,)),
            dma((2,)), dma((2,)),
            dma((9,)), dma((9,)),
            dma((2, 8)), dma((2, 8)),
            dma((8,)), dma((8,)),
            dma((3, 4)), dma((3, 4)),
            dma((15,)), dma((15,)),
            dma((24,)), dma((24,)),
            pltpu.SemaphoreType.REGULAR((3,)),
        ],
        compiler_params=pltpu.CompilerParams(
            collective_id=0, has_side_effects=True, vmem_limit_bytes=46 * 1024 * 1024
        ),
        cost_estimate=pl.CostEstimate(
            flops=2 * 896 * 1024 * 4096 + 2 * 2048 * 1024 * 768,
            bytes_accessed=10_000_000,
            transcendentals=0,
        ),
    )(
        pltpu.with_memory_space_constraint(slot_count[0, 0], pltpu.HBM),
        pltpu.with_memory_space_constraint(slot_gate[0, 0], pltpu.HBM),
        pltpu.with_memory_space_constraint(normed_inputs[0, 0].reshape(384, D), pltpu.HBM),
        pltpu.with_memory_space_constraint(value_cotangent[0, 0].reshape(384, KV), pltpu.HBM),
        pltpu.with_memory_space_constraint(expert_hidden[0, 0].reshape(4, 8, 32, 896), pltpu.HBM),
        pltpu.with_memory_space_constraint(expert_cotangent[0, 0], pltpu.HBM),
        pltpu.with_memory_space_constraint(expert_moment[0], pltpu.HBM),
        pltpu.with_memory_space_constraint(expert_weight[0], pltpu.HBM),
        pltpu.with_memory_space_constraint(value_moment[0], pltpu.HBM),
        pltpu.with_memory_space_constraint(value_weight[0], pltpu.HBM),
    )
    expert_weight_next, expert_next, value_weight_next, value_next = pl.pallas_call(
        update_kernel,
        name="update",
        out_shape=(
            jax.ShapeDtypeStruct((896, 1024), bf16),
            jax.ShapeDtypeStruct((896, 1024), jnp.float32),
            jax.ShapeDtypeStruct((128, 1024), bf16),
            jax.ShapeDtypeStruct((128, 1024), jnp.float32),
        ),
        in_specs=[vmem] * 4,
        out_specs=(in_hbm,) * 4,
        scratch_shapes=[
            pltpu.VMEM((1024, 1024), bf16),
            pltpu.VMEM((1024, 1024), jnp.float32),
            dma((1024 // TILE,)),
            dma((1024 // TILE,)),
        ],
        compiler_params=pltpu.CompilerParams(vmem_limit_bytes=24 * 1024 * 1024),
        cost_estimate=pl.CostEstimate(flops=6 * 1024 * 1024, bytes_accessed=6_000_000, transcendentals=0),
    )(
        factor, grads, moments, weights,
    )
    return (expert_weight_next[None], expert_next[None], value_weight_next[None], value_next[None])


def solution(mesh):
    finer = Mesh(mesh.devices.reshape(mesh.shape["section"], 4, 2, 2, 2), AXES)
    specs = (
        P("section", WIDE, NARROW),
        P("section", WIDE, NARROW),
        P("section", WIDE_NARROW, None),
        P("section", WIDE_NARROW, None),
    )
    in_specs = (
        P("section", NARROW, None, WIDE, None),
        P("section", NARROW, None, WIDE, None),
        P("section", NARROW, None, None, WIDE),
        P("section", NARROW, None, WIDE, None),
        P("section", NARROW, None, WIDE),
        P("section", NARROW, None),
    ) + specs
    return jax.shard_map(
        on_device, mesh=finer, in_specs=in_specs, out_specs=specs, check_vma=False
    )
```

```python
import math

import jax
import jax.numpy as jnp
from jax import lax
from jax.experimental import pallas as pl
from jax.experimental.pallas import tpu as pltpu
from jax.sharding import Mesh
from jax.sharding import PartitionSpec as P

D = 4096
FF = 7168
KV = 1024
SECTIONS = 4
ENTRY_COUNT = SECTIONS * (FF * D + D * KV)
AXES = ("section", "wide_0", "wide_1", "narrow_0", "narrow_1")
WIDE = ("wide_0", "wide_1")
NARROW = ("narrow_0", "narrow_1")
WIDE_NARROW = ("wide_0", "wide_1", "narrow_0", "narrow_1")
MESH = pl.DeviceIdType.MESH

TILE = 128

MOMENTUM_DECAY = 0.9
STEP_RATE = 0.01

PIECES = ((0, 0), (1, 0), (2, 0), (2, 1), (3, 0), (3, 1), (0, 1), (1, 1))
BY_Z1 = (0, 2, 4, 6)
BY_Z3 = (1, 3, 5, 7)


def flip(value, mask):
    if mask == 0:
        return value
    if mask == 1:
        return value + 1 - 2 * (value % 2)
    if mask == 2:
        return (value + 2) % 4
    return 3 - value


def kernel(
    counts, gates, inputs, value_cot, hidden, cotangent,
    expert_moment, expert_weight, value_moment, value_weight,
    grads_out, moments_out, weights_out, factor_out,
    count_ref, gate_ref, staged, gathered, relay, weights, tokens, token_cots, parts, halves, quarters, cross, eighths, last,
    norms,
    local_sem, token_send, token_recv, cot_send, cot_recv, z_send, z_recv, zf_send, zf_recv,
    hid_send, hid_recv, val_send, val_recv, norm_send, norm_recv, reach_sem,
):
    section = lax.axis_index("section")
    z = lax.axis_index("wide_0")
    hi = lax.axis_index("wide_1")
    lo = lax.axis_index("narrow_0")
    core = lax.axis_index("narrow_1")
    x = 2 * hi + lo
    side = (hi, 1 - hi)

    def device(dy=0, dz=0, dx=0, dc=0):
        there = flip(x, dx)
        return (flip(section, dy), flip(z, dz), there // 2, there % 2, 1 - core if dc else core)

    def send(src, dst, send_sem, recv_sem, **where):
        return pltpu.make_async_remote_copy(
            src_ref=src, dst_ref=dst, send_sem=send_sem, recv_sem=recv_sem,
            device_id=device(**where), device_id_type=MESH,
        )

    pending = []

    def start(copy):
        copy.start()
        pending.append(copy)
        return copy

    row_peers = [dict(dx=dx, dc=dc) for dx, dc in ((2, 1), (2, 0), (1, 1), (3, 1), (1, 0), (3, 0), (0, 1))]
    far_peers = [dict(dz=i % 4, dy=i // 4) for i in (10, 6, 14, 9, 11, 2, 8, 5, 7, 13, 15, 1, 3, 4, 12)]

    small_loads = [
        pltpu.make_async_copy(counts, count_ref, local_sem.at[10]),
        pltpu.make_async_copy(gates, gate_ref, local_sem.at[11]),
    ]
    for load in small_loads:
        load.start()
    cot_loads = []
    for rel in range(4):
        column = (2 * (1 - lo if rel // 2 else lo) + (1 - core if rel % 2 else core)) * 1024
        source = cotangent.at[:, :, pl.ds(pl.multiple_of(column, 1024), 1024)]
        load = pltpu.make_async_copy(source, staged.at[rel], local_sem.at[rel])
        load.start()
        cot_loads.append(load)
    barrier = pltpu.get_barrier_semaphore()
    near = [dict(dc=1), dict(dz=1), dict(dz=3), dict(dy=1), dict(dy=3)]
    near += [dict(dx=dx, dc=dc) for dx in (1, 3) for dc in (0, 1)]
    for peer in near:
        pl.semaphore_signal(barrier, inc=1, device_id=device(**peer), device_id_type=MESH)

    lanes = lax.broadcasted_iota(jnp.int32, (1, 32), 1) + (2 * z + hi) * 32
    diagonal = lax.broadcasted_iota(jnp.int32, (32, 32), 0) == lax.broadcasted_iota(
        jnp.int32, (32, 32), 1
    )
    columns = []
    for load in small_loads:
        load.wait()
    for micro in range(4):
        gate = gate_ref[micro : micro + 1, :].astype(jnp.float32)
        row = jnp.where(lanes < count_ref[micro], gate, jnp.zeros_like(gate))
        square = jnp.where(diagonal, jnp.broadcast_to(row, (32, 32)), 0.0)
        columns.append(jnp.sum(square, axis=1, keepdims=True))

    def scale(rel):
        cot_loads[rel].wait()
        for micro in range(4):
            scaled = (columns[micro] * staged[rel, micro].astype(jnp.float32)).astype(jnp.bfloat16)
            if rel == 0:
                gathered[0, 0, micro, hi] = scaled
            else:
                staged[rel, micro] = scaled

    def spread(step):
        if step:
            pl.semaphore_wait(reach_sem.at[step - 1], 4)
        if step < 3:
            for peer in near[1:5]:
                pl.semaphore_signal(
                    reach_sem.at[step], inc=1, device_id=device(**peer), device_id_type=MESH
                )

    def piece(slot, index):
        replica, far = PIECES[index]
        return gathered.at[slot, replica, :, side[far]]

    def along_z(index):
        start(send(piece(0, index), piece(1, index), z_send.at[0, index], z_recv.at[0, index], dz=1))
        start(send(piece(0, index), piece(3, index), z_send.at[1, index], z_recv.at[1, index], dz=3))

    def z_arrival(link, index):
        slot = (1, 3)[link]
        return send(piece(0, index), piece(slot, index), z_send.at[link, index], z_recv.at[link, index], dz=slot)

    def forward_z(index):
        if index in BY_Z1:
            z_arrival(1, index).wait_recv()
            start(send(piece(3, index), piece(2, index), zf_send.at[index], zf_recv.at[index], dz=1))
        else:
            z_arrival(0, index).wait_recv()
            start(send(piece(1, index), piece(2, index), zf_send.at[index], zf_recv.at[index], dz=3))

    def into(replica, far):
        return gathered.at[0, replica, :, side[far]]

    mine_0 = into(0, 0)
    cot = {}

    def cot_send_of(name, index, src, dst, **where):
        cot[name] = start(send(src, dst, cot_send.at[index], cot_recv.at[index], **where))

    scale(0)
    pl.semaphore_wait(barrier, len(near))
    scale(2)
    along_z(0)
    cot_send_of("x1_same", 3, staged.at[2], into(2, 0), dx=1)
    cot_send_of("x3_same", 4, staged.at[2], into(2, 0), dx=3)
    cot_send_of("relay_1", 1, mine_0, relay.at[0], dx=1)
    scale(1)
    scale(3)
    cot_send_of("core", 0, staged.at[1], into(1, 0), dc=1)
    cot_send_of("relay_3", 2, staged.at[1], relay.at[1], dx=3)
    cot_send_of("x1_cross", 5, staged.at[3], into(3, 0), dx=1, dc=1)
    cot_send_of("x3_cross", 6, staged.at[3], into(3, 0), dx=3, dc=1)

    load_cots = pltpu.make_async_copy(value_cot, token_cots.at[0], local_sem.at[4])
    load_cots.start()
    others = []
    for dx in range(4):
        for dz in range(4):
            block = 2 * (4 * flip(z, dz) + flip(x, dx))
            place = pl.ds((dx * 4 + dz) * 128, 128)
            for which, owner in ((0, core), (1, 1 - core)):
                source = inputs.at[:, pl.ds(pl.multiple_of((block + owner) * 128, 128), 128)]
                if which == 0:
                    pltpu.make_async_copy(source, tokens.at[0, :, place], local_sem.at[5]).start()
                else:
                    others.append((source, place))
    hid_loads = []
    for dz in range(4):
        rows = pl.ds(2 * flip(z, dz), 2)
        load = pltpu.make_async_copy(hidden.at[:, rows], weights.at[0, dz], local_sem.at[6 + dz])
        load.start()
        hid_loads.append(load)
    state_loads = [
        pltpu.make_async_copy(expert_moment, moments_out.at[0:896], local_sem.at[12]),
        pltpu.make_async_copy(expert_weight, weights_out.at[0:896], local_sem.at[13]),
        pltpu.make_async_copy(value_moment, moments_out.at[896:1024], local_sem.at[14]),
        pltpu.make_async_copy(value_weight, weights_out.at[896:1024], local_sem.at[15]),
    ]

    spread(0)
    for source, place in others:
        send(source, tokens.at[1, :, place], token_send.at[0], token_recv.at[0], dc=1).start()
    token_whole = send(tokens.at[1], tokens.at[1], token_send.at[0], token_recv.at[0], dc=1)
    pending.append(token_whole)
    cots_whole = start(send(value_cot, token_cots.at[1], token_send.at[1], token_recv.at[1], dc=1))
    hid_core = []
    for dz in range(4):
        rows = pl.ds(2 * flip(z, dz), 2)
        hid_core.append(
            start(send(hidden.at[:, rows], weights.at[1, dz], hid_send.at[0, dz], hid_recv.at[0, dz], dc=1))
        )

    cot["core"].wait_recv()
    along_z(1)

    load_cots.wait()
    pltpu.make_async_copy(tokens.at[0], tokens.at[0], local_sem.at[5]).wait()
    token_whole.wait_recv()
    cots_whole.wait_recv()

    def value_parts(dx):
        def block(dz, carry):
            place = pl.ds(pl.multiple_of((dx * 4 + dz) * 128, 128), 128)
            lhs = tokens[:, :, place].reshape(768, 128)
            rhs = token_cots[...].reshape(768, KV)
            product = lax.dot_general(
                lhs, rhs, (((0,), (0,)), ((), ())), preferred_element_type=jnp.float32
            )
            parts[dx, dz] = product.astype(jnp.bfloat16)
            return carry

        lax.fori_loop(0, 4, block, 0)

    value = {}

    def value_send(name, index, src, dst, **where):
        value[name] = start(send(src, dst, val_send.at[index], val_recv.at[index], **where))

    hid_far = {}

    def send_hidden(dz):
        hid_loads[dz].wait()
        hid_far[dz] = start(
            send(weights.at[0, dz], weights.at[2, dz], hid_send.at[1, dz], hid_recv.at[1, dz], dx=1)
        )

    value_parts(2)
    cot["x1_same"].wait_recv()
    along_z(2)
    cot["x3_same"].wait_recv()
    along_z(3)
    value_parts(3)
    cot["relay_1"].wait_recv()
    cot_send_of("far_3", 7, relay.at[0], into(0, 0), dx=3)
    cot["relay_3"].wait_recv()
    cot_send_of("far_1", 8, relay.at[1], into(1, 1), dx=1, dc=1)
    for dz in (0, 1, 3):
        send_hidden(dz)
    for i, (far, dz) in enumerate(((1, 2), (0, 2), (1, 1), (1, 3), (1, 0), (0, 3), (0, 1), (0, 0))):
        value_send(("x3", far, dz), i, parts.at[3 - far, dz], halves.at[far, dz], dx=3)
    for load in state_loads:
        load.start()
    spread(1)
    value_parts(1)
    cot["x1_cross"].wait_recv()
    along_z(4)
    cot["x3_cross"].wait_recv()
    along_z(5)
    value_parts(0)
    spread(2)
    cot["far_3"].wait_recv()
    along_z(6)
    cot["far_1"].wait_recv()
    along_z(7)

    def accumulate(weights_of, gathered_of, first=False):
        def tile(n, carry):
            place = pl.ds(pl.multiple_of(n * 512, 512), 512)
            lhs = weights_of().reshape(256, 896)
            rhs = gathered_of(place).reshape(256, 512)
            product = lax.dot_general(
                lhs, rhs, (((0,), (0,)), ((), ())), preferred_element_type=jnp.float32
            )
            if first:
                grads_out[0:896, place] = product
            else:
                grads_out[0:896, place] += product
            return carry

        lax.fori_loop(0, 2, tile, 0)

    def products(slot, replica, first=False):
        accumulate(
            lambda: weights[replica, slot],
            lambda place: gathered[slot, replica, :, :, :, place],
            first,
        )

    def chip_products(slot, far):
        accumulate(
            lambda: weights[0:2, slot, :, side[far]],
            lambda place: gathered[slot, 0:2, :, side[far], :, place],
        )

    def second_step(dz, more=None):
        value[("x3", 1, dz)].wait_recv()
        total = parts[1, dz].astype(jnp.float32) + halves[1, dz].astype(jnp.float32)
        if more is not None:
            total = total + more[...].astype(jnp.float32)
        parts[1, dz] = total.astype(jnp.bfloat16)

    def second_send(dz):
        value_send(("x1", dz), 8 + dz, parts.at[1, dz], quarters.at[dz], dx=1)

    hid_pass = {}

    def pass_hidden(dz):
        hid_far[dz].wait_recv()
        hid_pass[dz] = start(
            send(weights.at[2, dz], weights.at[3, dz], hid_send.at[2, dz], hid_recv.at[2, dz], dc=1)
        )

    def far_arrival(index):
        if index in BY_Z1:
            send(piece(3, index), piece(2, index), zf_send.at[index], zf_recv.at[index], dz=1).wait_recv()
        else:
            send(piece(1, index), piece(2, index), zf_send.at[index], zf_recv.at[index], dz=3).wait_recv()

    def third_step(dz):
        value[("x3", 0, dz)].wait_recv()
        total = parts[0, dz].astype(jnp.float32) + halves[0, dz].astype(jnp.float32)
        if dz != 2:
            value[("x1", dz)].wait_recv()
            total = total + quarters[dz].astype(jnp.float32)
        return total

    products(0, 0, first=True)
    second_step(2)
    hid_core[0].wait_recv()
    products(0, 1)
    value_send("cross", 10, parts.at[1, 2], cross, dz=3)
    parts[0, 2] = third_step(2).astype(jnp.bfloat16)
    forward_z(0)
    forward_z(1)
    value_send("z1_1", 13, parts.at[0, 2], eighths.at[1], dz=1)
    forward_z(2)
    forward_z(3)
    forward_z(4)
    pass_hidden(0)
    products(0, 2)
    forward_z(5)
    hid_pass[0].wait_recv()
    products(0, 3)
    forward_z(6)
    pass_hidden(1)
    second_step(3)
    forward_z(7)
    drained = len(pending)
    second_send(3)
    z_arrival(0, 0).wait_recv()
    z_arrival(0, 6).wait_recv()
    products(1, 0)
    second_step(0)
    value["cross"].wait_recv()
    second_step(1, cross)
    hid_core[1].wait_recv()
    z_arrival(1, 1).wait_recv()
    z_arrival(1, 7).wait_recv()
    products(1, 1)
    second_send(1)
    send_hidden(2)
    second_send(0)
    z_arrival(0, 2).wait_recv()
    products(1, 2)
    pass_hidden(3)
    hid_pass[1].wait_recv()
    z_arrival(0, 4).wait_recv()
    products(1, 3)
    third = third_step(3)
    value["z1_1"].wait_recv()
    parts[0, 3] = (third + eighths[1].astype(jnp.float32)).astype(jnp.bfloat16)
    products(3, 0)
    value_send("z3", 14, parts.at[0, 3], last, dz=3)
    parts[0, 1] = third_step(1).astype(jnp.bfloat16)
    hid_core[3].wait_recv()
    products(3, 1)
    value_send("z1_0", 12, parts.at[0, 1], eighths.at[0], dz=1)
    z_arrival(1, 3).wait_recv()
    products(3, 2)
    hid_pass[3].wait_recv()
    z_arrival(1, 5).wait_recv()
    products(3, 3)
    hid_core[2].wait_recv()
    far_arrival(0)
    far_arrival(1)
    chip_products(2, 0)
    pass_hidden(2)
    far_arrival(2)
    far_arrival(3)
    products(2, 2)
    hid_pass[2].wait_recv()
    far_arrival(4)
    far_arrival(5)
    products(2, 3)
    for copy in pending[:drained]:
        copy.wait_send()
    far_arrival(6)
    far_arrival(7)
    chip_products(2, 1)

    def squares(first, rows):
        def tile(i, totals):
            chunk = grads_out[pl.ds(pl.multiple_of(first + i * 32, 32), 32), :]
            totals = list(totals)
            for group in range(4):
                for n in range(8):
                    one = chunk[group * 8 : (group + 1) * 8, n * 128 : (n + 1) * 128]
                    totals[n] = totals[n] + one * one
            return tuple(totals)

        totals = lax.fori_loop(0, rows // 32, tile, (jnp.zeros((8, 128), jnp.float32),) * 8)
        return sum(totals[1:], totals[0])

    spread(3)
    expert_squares = squares(0, 896)
    for load in state_loads:
        load.wait()
    near = third_step(0)
    value["z1_0"].wait_recv()
    near = near + eighths[0].astype(jnp.float32)
    value["z3"].wait_recv()
    grads_out[896:1024, :] = near + last[...].astype(jnp.float32)
    norms[0] = jnp.sum(expert_squares + squares(896, 128), axis=0, keepdims=True)
    started = len(pending)

    base = 0
    slot = 1
    for group in (row_peers, far_peers):
        copies = []
        for i, peer in enumerate(group):
            copies.append(
                start(
                    send(norms.at[base], norms.at[slot + i], norm_send.at[slot + i], norm_recv.at[slot + i], **peer)
                )
            )
        if base == 0:
            for copy in pending[drained:started]:
                copy.wait_send()
        total = norms[base]
        for i, copy in reversed(tuple(enumerate(copies))):
            copy.wait_recv()
            total = total + norms[slot + i]
        base = slot + len(group)
        norms[base] = total
        slot = base + 1
    overall = jnp.sum(norms[base], axis=1, keepdims=True)
    overall = jnp.broadcast_to(overall, (8, 128))
    factor_out[...] = jnp.minimum(1.0, math.sqrt(ENTRY_COUNT) / jnp.sqrt(overall + 1e-06))

    for copy in pending[started:]:
        copy.wait_send()


def update_kernel(
    factor_ref, grads, moments, weights,
    expert_weight_out, expert_moment_out, value_weight_out, value_moment_out,
    new_weights, new_moments, weight_sem, moment_sem,
):
    factor = factor_ref[0:1, 0:1]
    copies = []
    for tile in range(1024 // TILE):

        def chunk(i, carry, tile=tile):
            at = pl.ds(pl.multiple_of(tile * TILE + i * 32, 32), 32)
            moved = MOMENTUM_DECAY * moments[at, :] + factor * grads[at, :]
            new_moments[at, :] = moved
            new_weights[at, :] = (weights[at, :].astype(jnp.float32) - STEP_RATE * moved).astype(
                jnp.bfloat16
            )
            return carry

        lax.fori_loop(0, TILE // 32, chunk, 0)
        rows = pl.ds(tile * TILE, TILE)
        expert = tile * TILE < 896
        there = rows if expert else pl.ds(tile * TILE - 896, TILE)
        outs = (expert_weight_out, expert_moment_out) if expert else (value_weight_out, value_moment_out)
        for src, dst, sem in (
            (new_weights, outs[0], weight_sem),
            (new_moments, outs[1], moment_sem),
        ):
            copy = pltpu.make_async_copy(src.at[rows, :], dst.at[there, :], sem.at[tile])
            copy.start()
            copies.append(copy)
    for copy in copies:
        copy.wait()


def on_device(
    normed_inputs, value_cotangent, expert_hidden, expert_cotangent, slot_gate, slot_count,
    expert_weight, expert_moment, value_weight, value_moment,
):
    bf16 = jnp.bfloat16
    in_hbm = pl.BlockSpec(memory_space=pltpu.HBM)
    vmem = pl.BlockSpec(memory_space=pltpu.VMEM)
    dma = pltpu.SemaphoreType.DMA
    grads, moments, weights, factor = pl.pallas_call(
        kernel,
        name="gradients",
        out_shape=(
            pltpu.VMEM((1024, 1024), jnp.float32),
            pltpu.VMEM((1024, 1024), jnp.float32),
            pltpu.VMEM((1024, 1024), bf16),
            pltpu.VMEM((8, 128), jnp.float32),
        ),
        in_specs=[in_hbm] * 10,
        out_specs=(vmem,) * 4,
        scratch_shapes=[
            pltpu.SMEM((4,), jnp.int32),
            pltpu.VMEM((4, 32), bf16),
            pltpu.VMEM((4, 4, 32, 1024), bf16),
            pltpu.VMEM((4, 4, 4, 2, 32, 1024), bf16),
            pltpu.VMEM((2, 4, 32, 1024), bf16),
            pltpu.VMEM((4, 4, 4, 2, 32, 896), bf16),
            pltpu.VMEM((2, 384, 2048), bf16),
            pltpu.VMEM((2, 384, 1024), bf16),
            pltpu.VMEM((4, 4, 128, 1024), bf16),
            pltpu.VMEM((2, 4, 128, 1024), bf16),
            pltpu.VMEM((4, 128, 1024), bf16),
            pltpu.VMEM((128, 1024), bf16),
            pltpu.VMEM((2, 128, 1024), bf16),
            pltpu.VMEM((128, 1024), bf16),
            pltpu.VMEM((25, 1, 128), jnp.float32),
            dma((16,)),
            dma((2,)), dma((2,)),
            dma((9,)), dma((9,)),
            dma((2, 8)), dma((2, 8)),
            dma((8,)), dma((8,)),
            dma((3, 4)), dma((3, 4)),
            dma((15,)), dma((15,)),
            dma((24,)), dma((24,)),
            pltpu.SemaphoreType.REGULAR((3,)),
        ],
        compiler_params=pltpu.CompilerParams(
            collective_id=0, has_side_effects=True, vmem_limit_bytes=46 * 1024 * 1024
        ),
        cost_estimate=pl.CostEstimate(
            flops=2 * 896 * 1024 * 4096 + 2 * 2048 * 1024 * 768,
            bytes_accessed=10_000_000,
            transcendentals=0,
        ),
    )(
        pltpu.with_memory_space_constraint(slot_count[0, 0], pltpu.HBM),
        pltpu.with_memory_space_constraint(slot_gate[0, 0], pltpu.HBM),
        pltpu.with_memory_space_constraint(normed_inputs[0, 0].reshape(384, D), pltpu.HBM),
        pltpu.with_memory_space_constraint(value_cotangent[0, 0].reshape(384, KV), pltpu.HBM),
        pltpu.with_memory_space_constraint(expert_hidden[0, 0].reshape(4, 8, 32, 896), pltpu.HBM),
        pltpu.with_memory_space_constraint(expert_cotangent[0, 0], pltpu.HBM),
        pltpu.with_memory_space_constraint(expert_moment[0], pltpu.HBM),
        pltpu.with_memory_space_constraint(expert_weight[0], pltpu.HBM),
        pltpu.with_memory_space_constraint(value_moment[0], pltpu.HBM),
        pltpu.with_memory_space_constraint(value_weight[0], pltpu.HBM),
    )
    expert_weight_next, expert_next, value_weight_next, value_next = pl.pallas_call(
        update_kernel,
        name="update",
        out_shape=(
            jax.ShapeDtypeStruct((896, 1024), bf16),
            jax.ShapeDtypeStruct((896, 1024), jnp.float32),
            jax.ShapeDtypeStruct((128, 1024), bf16),
            jax.ShapeDtypeStruct((128, 1024), jnp.float32),
        ),
        in_specs=[vmem] * 4,
        out_specs=(in_hbm,) * 4,
        scratch_shapes=[
            pltpu.VMEM((1024, 1024), bf16),
            pltpu.VMEM((1024, 1024), jnp.float32),
            dma((1024 // TILE,)),
            dma((1024 // TILE,)),
        ],
        compiler_params=pltpu.CompilerParams(vmem_limit_bytes=24 * 1024 * 1024),
        cost_estimate=pl.CostEstimate(flops=6 * 1024 * 1024, bytes_accessed=6_000_000, transcendentals=0),
    )(
        factor, grads, moments, weights,
    )
    return (expert_weight_next[None], expert_next[None], value_weight_next[None], value_next[None])


def solution(mesh):
    finer = Mesh(mesh.devices.reshape(mesh.shape["section"], 4, 2, 2, 2), AXES)
    specs = (
        P("section", WIDE, NARROW),
        P("section", WIDE, NARROW),
        P("section", WIDE_NARROW, None),
        P("section", WIDE_NARROW, None),
    )
    in_specs = (
        P("section", NARROW, None, WIDE, None),
        P("section", NARROW, None, WIDE, None),
        P("section", NARROW, None, None, WIDE),
        P("section", NARROW, None, WIDE, None),
        P("section", NARROW, None, WIDE),
        P("section", NARROW, None),
    ) + specs
    return jax.shard_map(
        on_device, mesh=finer, in_specs=in_specs, out_specs=specs, check_vma=False
    )
```
